32 devices in a mesh: dp: 4 (over x, core), fsdp: 8 (over z, y).
Axes of the slice: x: 2, y: 2, z: 4, core: 2. Of those that a mesh axis runs over, the one named last changes fastest.
Arguments:
- frames: bfloat16 [8, 1024, 1024], P('fsdp', 'dp'), may hold values from -6 to 6
- cotangent: bfloat16 [8, 1024, 1024], P('fsdp', 'dp'), may hold values from -6 to 6
- phon_len: int32 [8], replicated, may hold values from 32 to 128
- acou_len: int32 [8], replicated, may hold values from 128 to 895
- row_item: int32 [8], P('fsdp'), may hold values from 0 to 7, each once
- w_qkv: bfloat16 [1024, 3072], P(('dp', 'fsdp')), may hold values from -0.1875 to 0.1875
- w_out: bfloat16 [1024, 1024], P(('dp', 'fsdp')), may hold values from -2 to 2
- w_up: bfloat16 [1024, 4096], P(('dp', 'fsdp')), may hold values from -0.1875 to 0.1875
- w_down: bfloat16 [4096, 1024], P(('dp', 'fsdp')), may hold values from -0.09375 to 0.09375
- ln1_gain: bfloat16 [1024], P(('dp', 'fsdp')), may hold values from 0.25 to 1.75
- ln1_bias: bfloat16 [1024], P(('dp', 'fsdp')), may hold values from -2.5 to 2.5
- ln2_gain: bfloat16 [1024], P(('dp', 'fsdp')), may hold values from 0.25 to 1.75
- ln2_bias: bfloat16 [1024], P(('dp', 'fsdp')), may hold values from -2.5 to 2.5
Outputs:
- activations: bfloat16 [8, 1024, 1024], P('fsdp', 'dp')
- input_grad: float32 [8, 1024, 1024], P('fsdp', 'dp')
- w_qkv_grad: float32 [1024, 3072], P(('dp', 'fsdp'))
- w_out_grad: float32 [1024, 1024], P(('dp', 'fsdp'))
- w_up_grad: float32 [1024, 4096], P(('dp', 'fsdp'))
- w_down_grad: float32 [4096, 1024], P(('dp', 'fsdp'))
- ln1_gain_grad: float32 [1024], P(('dp', 'fsdp'))
- ln1_bias_grad: float32 [1024], P(('dp', 'fsdp'))
- ln2_gain_grad: float32 [1024], P(('dp', 'fsdp'))
- ln2_bias_grad: float32 [1024], P(('dp', 'fsdp'))
The draws below stay inside these ranges and needn't reach their ends.
Inputs may be any that keep to these rules, and one draw needn't show every extreme that they name: `acou_len`: an item's phoneme and acoustic lengths together are under 1024. `row_item`: each row holds a different item.
All inputs are finite; a program needn't handle non-finite values.
Results may differ from the reference program's by a relative error of at most 0.011.
Values may be sent and summed in bfloat16 or wider, within the bound.
A program may use at most 256 MiB of HBM per device.

```python
import jax
import jax.numpy as jnp
from jax import lax

D = 1024
HEADS = 16
HEAD_DIM = 64
FF = 4096
LEN = 1024
ROWS = 8


def touch_ends(result, own_key, low, high):
    longest = result.shape.index(max(result.shape))
    spots = []
    for shift in (0, 1):
        where = [jax.random.randint(jax.random.fold_in(own_key, axis), (), 0, length) for axis, length in enumerate(result.shape)]
        where[longest] = (where[longest] + shift) % result.shape[longest]
        spots.append(tuple(where))
    return result.at[spots[0]].set(low).at[spots[1]].set(high)


def level_of(own_key, dims, cuts, low, largest):
    factor_of, own = 1.0, jax.random.fold_in(own_key, 6)
    for dim, parts in cuts:
        draws = jnp.exp(jax.random.uniform(jax.random.fold_in(own, dim), (parts,), jnp.float32, low / len(cuts), largest / len(cuts)))
        factor_of = factor_of * jnp.repeat(draws, dims[dim] // parts).reshape([-1 if axis == dim else 1 for axis in range(len(dims))])
    return factor_of


def scatter_about(rng, dims, spread, bound, cuts=(), held_as=jnp.bfloat16):
    result = jax.random.normal(rng, dims, jnp.float32) * spread
    if len(cuts) > 0:
        result = level_of(rng, dims, cuts, -0.22, 0.18) * result
    return jnp.clip(result, min=-bound, max=bound).astype(held_as)


def setup_inputs(seed: int = 0) -> dict:
    arg_keys = jax.random.split(jax.random.key(seed), 14)
    frames = scatter_about(arg_keys[0], (ROWS, LEN, D), 1.0, 6.0, ((0, 8), (1, 4)))
    cotangent = scatter_about(arg_keys[1], (ROWS, LEN, D), 1.0, 6.0, ((0, 8), (1, 4)))
    phon_len = touch_ends(jax.random.randint(arg_keys[2], (ROWS,), LEN // 32, LEN // 8 + 1), jax.random.fold_in(arg_keys[2], 1), LEN // 32, (LEN // 8 + 1) - 1).astype(jnp.int32)
    acou_len = touch_ends(jax.random.randint(arg_keys[3], (ROWS,), LEN // 8, LEN - LEN // 8), jax.random.fold_in(arg_keys[3], 1), LEN // 8, (LEN - LEN // 8) - 1).astype(jnp.int32)
    row_item = jax.random.permutation(arg_keys[4], ROWS).astype(jnp.int32)
    w_qkv = scatter_about(arg_keys[5], (D, 3 * D), D ** -0.5, 0.1875, ((0, 32),))
    w_out = scatter_about(arg_keys[6], (D, D), (D // 128) ** -0.5, 2.0, ((0, 32),))
    w_up = scatter_about(arg_keys[7], (D, FF), D ** -0.5, 0.1875, ((0, 32),))
    w_down = scatter_about(arg_keys[8], (FF, D), FF ** -0.5, 0.09375, ((0, 32),))
    ln1_gain = jnp.clip(1.0 + 0.15 * jax.random.normal(arg_keys[9], (D,), jnp.float32), 0.25, 1.75).astype(jnp.bfloat16)
    ln1_bias = scatter_about(arg_keys[10], (D,), 0.5, 2.5, ((0, 32),))
    ln2_gain = jnp.clip(1.0 + 0.15 * jax.random.normal(arg_keys[11], (D,), jnp.float32), 0.25, 1.75).astype(jnp.bfloat16)
    ln2_bias = scatter_about(arg_keys[12], (D,), 0.5, 2.5, ((0, 32),))
    return {"frames": frames, "cotangent": cotangent, "phon_len": phon_len, "acou_len": acou_len, "row_item": row_item, "w_qkv": w_qkv, "w_out": w_out, "w_up": w_up, "w_down": w_down, "ln1_gain": ln1_gain, "ln1_bias": ln1_bias, "ln2_gain": ln2_gain, "ln2_bias": ln2_bias}


@jax.custom_vjp
def low(v):
    return lax.optimization_barrier(v.astype(jnp.bfloat16)).astype(jnp.float32)

@jax.custom_vjp
def low_back(v):
    return v

def low_keep(v):
    return (low(v), None)

def low_pass(kept, grad):
    return (grad,)

def back_keep(v):
    return (v, None)

def back_low(kept, grad):
    return (low(grad),)
low.defvjp(low_keep, low_pass)
low_back.defvjp(back_keep, back_low)
epsilon = 1e-05
masked_out = -1e+30

def layer_norm(vector, gain_vec, bias_vec):
    row_mean = lax.optimization_barrier(jnp.mean(vector, axis=-1, keepdims=True))
    centered = vector - row_mean
    row_var = lax.optimization_barrier(jnp.mean(centered * centered, axis=-1, keepdims=True))
    return centered * lax.rsqrt(row_var + epsilon) * gain_vec + bias_vec

def matmul(left, right):
    return jnp.dot(left, right, precision=lax.Precision.HIGHEST)

def row_forward(frames_row, phon_count, acou_count, w_qkv, w_out, w_up, w_down, gain_one, bias_one, gain_two, bias_two):
    model_width = HEADS * HEAD_DIM
    row_length = frames_row.shape[0]
    normed1 = low(layer_norm(frames_row, gain_one, bias_one))
    qkv = low_back(low(matmul(normed1, w_qkv)))
    query = qkv[:, :model_width].reshape(row_length, HEADS, HEAD_DIM).transpose(1, 0, 2)
    keys_all = qkv[:, model_width:2 * model_width].reshape(row_length, HEADS, HEAD_DIM).transpose(1, 0, 2)
    values_all = qkv[:, 2 * model_width:].reshape(row_length, HEADS, HEAD_DIM).transpose(1, 0, 2)
    block_rows = min(512, row_length)
    block_count = row_length // block_rows
    key_pos = jnp.arange(row_length, dtype=jnp.int32)
    score_scale = HEAD_DIM ** (-0.5)

    def attend(pieces):
        q_block, start = pieces
        row_pos = start + jnp.arange(block_rows, dtype=jnp.int32)
        scores = jnp.einsum('hqd,hkd->hqk', q_block, keys_all, precision=lax.Precision.HIGHEST) * score_scale
        scores = low_back(scores)
        allowed = (key_pos[None, :] < phon_count) | (key_pos[None, :] >= phon_count) & (key_pos[None, :] <= row_pos[:, None]) & (row_pos[:, None] < phon_count + acou_count)
        scores = jnp.where(allowed[None], scores, masked_out)
        probs = low(jax.nn.softmax(scores, axis=-1))
        return jnp.einsum('hqk,hkd->hqd', probs, values_all, precision=lax.Precision.HIGHEST)
    q_blocks = query.reshape(HEADS, block_count, block_rows, HEAD_DIM).transpose(1, 0, 2, 3)
    starts = (jnp.arange(block_count, dtype=jnp.int32) * block_rows).astype(jnp.int32)
    head_out = lax.map(jax.checkpoint(attend), (q_blocks, starts))
    attn_out = head_out.transpose(0, 2, 1, 3).reshape(row_length, model_width)
    attn_out = low_back(low(attn_out))
    middle = frames_row + low_back(matmul(attn_out, w_out))
    normed2 = low(layer_norm(middle, gain_two, bias_two))
    up_out = low_back(matmul(normed2, w_up))
    act_out = low(jax.nn.gelu(up_out, approximate=False))
    return middle + low_back(matmul(act_out, w_down))

def reference(frames, cotangent, phon_len, acou_len, row_item, w_qkv, w_out, w_up, w_down, ln1_gain, ln1_bias, ln2_gain, ln2_bias):
    phon_rows = jnp.take(phon_len, row_item)
    acou_rows = jnp.take(acou_len, row_item)
    params = tuple((p.astype(jnp.float32) for p in (w_qkv, w_out, w_up, w_down, ln1_gain, ln1_bias, ln2_gain, ln2_bias)))

    def forward(inputs, wa, wb, wc, wd, ga, ba, gb, bb):

        def one_row(pieces):
            return row_forward(pieces[0], pieces[1], pieces[2], wa, wb, wc, wd, ga, ba, gb, bb)
        return lax.map(jax.checkpoint(one_row), (inputs, phon_rows, acou_rows))
    output, pullback = jax.vjp(forward, frames.astype(jnp.float32), *params)
    grads = pullback(cotangent.astype(jnp.float32))
    return (output.astype(jnp.bfloat16), grads[0], grads[1], grads[2], grads[3], grads[4], grads[5], grads[6], grads[7], grads[8])
```

```python
import functools

import jax
import jax.numpy as jnp
from jax import lax
from jax.experimental import pallas as pl
from jax.experimental.pallas import tpu as pltpu
from jax.sharding import PartitionSpec as P

HEAD_DIM = 64
EPS = 1e-05
MASKED = -1e30
BLOCK = 256

f32 = jnp.float32
bf16 = jnp.bfloat16


def dot(a, b, ca, cb):
    return lax.dot_general(a, b, (((ca,), (cb,)), ((), ())), preferred_element_type=f32)


def row_limit(start, rows, phon, acou):
    pos = start + lax.broadcasted_iota(jnp.int32, (1, rows), 1)
    return jnp.where(pos < phon + acou, jnp.maximum(pos, phon - 1), phon - 1)


def head_mask(width, head):
    lane = lax.broadcasted_iota(jnp.int32, (1, width), 1)
    return (lane >= head * HEAD_DIM) & (lane < (head + 1) * HEAD_DIM)


def attn_fwd_kernel(lens, qkv, out, lse):
    width = out.shape[1]
    heads = width // HEAD_DIM
    length = out.shape[0]
    phon, acou = lens[0], lens[1]
    scale = HEAD_DIM ** (-0.5)
    for start in range(0, length, BLOCK):
        seen = start + BLOCK
        q = qkv[start : start + BLOCK, :width] * scale
        k = qkv[:seen, width : 2 * width]
        v = qkv[:seen, 2 * width :]
        limit = row_limit(start, BLOCK, phon, acou)
        key = lax.broadcasted_iota(jnp.int32, (seen, 1), 0)
        hidden = key > limit
        total = jnp.zeros((BLOCK, width), f32)
        rows = []
        for h in range(heads):
            mine = head_mask(width, h)
            qh = jnp.where(mine, q, 0)
            s = dot(k, qh, 1, 1)
            s = jnp.where(hidden, MASKED, s)
            top = jnp.max(s, axis=0, keepdims=True)
            e = jnp.exp(s - top)
            tot = jnp.sum(e, axis=0, keepdims=True)
            p = (e * (1.0 / tot)).astype(bf16)
            o = dot(p, v, 0, 0)
            total = total + jnp.where(mine, o, 0)
            rows.append(top + jnp.log(tot))
        out[start : start + BLOCK, :] = total.astype(bf16)
        lse[:, start : start + BLOCK] = jnp.concatenate(rows + [jnp.zeros((8 - heads, BLOCK), f32)], axis=0)


def attn_bwd_kernel(lens, qkv, grad, lse, dqkv, dk_acc, dv_acc):
    width = grad.shape[1]
    heads = width // HEAD_DIM
    length = grad.shape[0]
    phon, acou = lens[0], lens[1]
    scale = HEAD_DIM ** (-0.5)
    for start in reversed(range(0, length, BLOCK)):
        seen = start + BLOCK
        q = qkv[start : start + BLOCK, :width] * scale
        g = grad[start : start + BLOCK, :]
        k = qkv[:seen, width : 2 * width]
        v = qkv[:seen, 2 * width :]
        limit = row_limit(start, BLOCK, phon, acou)
        key = lax.broadcasted_iota(jnp.int32, (seen, 1), 0)
        hidden = key > limit
        dq = jnp.zeros((BLOCK, width), f32)
        for h in range(heads):
            mine = head_mask(width, h)
            qh = jnp.where(mine, q, 0)
            gh = jnp.where(mine, g, 0)
            s = dot(k, qh, 1, 1)
            s = jnp.where(hidden, MASKED, s)
            p = jnp.exp(s - lse[h : h + 1, start : start + BLOCK])
            gp = dot(v, gh, 1, 1)
            delta = jnp.sum(p * gp, axis=0, keepdims=True)
            ds = (p * (gp - delta)).astype(bf16)
            dvh = dot(p.astype(bf16), gh, 1, 0)
            dkh = dot(ds, qh, 1, 0)
            if start == length - BLOCK and h == 0:
                dv_acc[...] = dvh
                dk_acc[...] = dkh
            else:
                dv_acc[:seen, :] += dvh
                dk_acc[:seen, :] += dkh
            dq = dq + jnp.where(mine, dot(ds, k, 0, 0), 0)
        dqkv[start : start + BLOCK, :width] = (dq * scale).astype(bf16)
    dqkv[:, width : 2 * width] = dk_acc[...].astype(bf16)
    dqkv[:, 2 * width :] = dv_acc[...].astype(bf16)


VMEM = pl.BlockSpec(memory_space=pltpu.VMEM)
SMEM = pl.BlockSpec(memory_space=pltpu.SMEM)


def attn_fwd(lens, qkv):
    length, width = qkv.shape[0], qkv.shape[1] // 3
    return pl.pallas_call(
        attn_fwd_kernel,
        out_shape=(jax.ShapeDtypeStruct((length, width), bf16), jax.ShapeDtypeStruct((8, length), f32)),
        in_specs=[SMEM, VMEM],
        out_specs=(VMEM, VMEM),
        compiler_params=pltpu.CompilerParams(vmem_limit_bytes=40 * 2**20),
        cost_estimate=pl.CostEstimate(flops=4 * length * length * width, bytes_accessed=8 * length * width, transcendentals=length * length * width // HEAD_DIM),
        name="attn_fwd",
    )(lens, qkv)


def attn_bwd(lens, qkv, grad, lse):
    length, width = grad.shape
    return pl.pallas_call(
        attn_bwd_kernel,
        out_shape=jax.ShapeDtypeStruct((length, 3 * width), bf16),
        in_specs=[SMEM, VMEM, VMEM, VMEM],
        out_specs=VMEM,
        scratch_shapes=[pltpu.VMEM((length, width), f32), pltpu.VMEM((length, width), f32)],
        compiler_params=pltpu.CompilerParams(vmem_limit_bytes=40 * 2**20),
        cost_estimate=pl.CostEstimate(flops=10 * length * length * width, bytes_accessed=14 * length * width, transcendentals=length * length * width // HEAD_DIM),
        name="attn_bwd",
    )(lens, qkv, grad, lse)


def norm_parts(v):
    mean = jnp.mean(v, axis=-1, keepdims=True)
    centered = v - mean
    var = jnp.mean(centered * centered, axis=-1, keepdims=True)
    inv = lax.rsqrt(var + EPS)
    return centered * inv, inv


def norm_back(n, inv, gain, grad):
    g = grad * gain
    dx = inv * (g - jnp.mean(g, axis=-1, keepdims=True) - n * jnp.mean(g * n, axis=-1, keepdims=True))
    return dx, jnp.sum(grad * n, axis=0), jnp.sum(grad, axis=0)


def on_device(frames, cotangent, phon_len, acou_len, row_item, w_qkv, w_out, w_up, w_down, ln1_gain, ln1_bias, ln2_gain, ln2_bias):
    tp, dpn, fsn = "dp", lax.axis_size("dp"), lax.axis_size("fsdp")
    width = frames.shape[2]
    part = width // dpn
    rows = w_up.shape[0]

    vecs = jnp.concatenate([ln1_gain, ln1_bias, ln2_gain, ln2_bias])[None]
    vecs = lax.all_gather(vecs, ("dp", "fsdp"), axis=0, tiled=True)
    vecs = vecs.reshape(dpn * fsn, 4, rows).transpose(1, 0, 2).reshape(4, width).astype(f32)

    qkv_cols = w_qkv.reshape(rows, 3, dpn, part).transpose(2, 0, 1, 3).reshape(dpn, rows, 3 * part)
    qkv_cols = lax.all_to_all(qkv_cols, tp, 0, 0, tiled=True)
    wq = lax.all_gather(qkv_cols, "fsdp", axis=1, tiled=True).reshape(width, 3 * part)
    wo = lax.all_gather(w_out, "fsdp", axis=0, tiled=True)
    ff = w_up.shape[1] // dpn
    up_cols = w_up.reshape(rows, dpn, ff).transpose(1, 0, 2)
    up_cols = lax.all_to_all(up_cols, tp, 0, 0, tiled=True)
    wu = lax.all_gather(up_cols, "fsdp", axis=1, tiled=True).reshape(width, ff)
    wd = lax.all_gather(w_down, "fsdp", axis=0, tiled=True)

    item = row_item[0]
    pick = jnp.arange(phon_len.shape[0], dtype=jnp.int32) == item
    lens = jnp.stack([jnp.sum(jnp.where(pick, phon_len, 0)), jnp.sum(jnp.where(pick, acou_len, 0))])

    x = frames[0].astype(f32)
    n1, inv1 = norm_parts(x)
    normed1 = lax.all_gather((n1 * vecs[0] + vecs[1]).astype(bf16), tp, axis=0, tiled=True)
    grad_down = lax.all_gather(cotangent[0], tp, axis=0, tiled=True)
    qkv = jnp.dot(normed1, wq, preferred_element_type=f32).astype(bf16)
    attn_out, lse = attn_fwd(lens, qkv)
    proj = jnp.dot(attn_out, wo, preferred_element_type=f32).astype(bf16)
    middle = x + lax.psum_scatter(proj, tp, scatter_dimension=0, tiled=True).astype(f32)
    n2, inv2 = norm_parts(middle)
    normed2 = lax.all_gather((n2 * vecs[2] + vecs[3]).astype(bf16), tp, axis=0, tiled=True)
    up_out = jnp.dot(normed2, wu, preferred_element_type=f32)
    cdf = 0.5 * (1.0 + lax.erf(up_out * (0.5**0.5)))
    act_out = (up_out * cdf).astype(bf16)
    down = jnp.dot(act_out, wd, preferred_element_type=f32).astype(bf16)
    result = (middle + lax.psum_scatter(down, tp, scatter_dimension=0, tiled=True).astype(f32)).astype(bf16)

    g_down = dot(act_out, grad_down, 0, 0).astype(bf16)
    slope = cdf + up_out * (jnp.exp(-0.5 * up_out * up_out) * (1.0 / (2.0 * jnp.pi) ** 0.5))
    grad_up = (dot(grad_down, wd, 1, 1) * slope).astype(bf16)
    g_up = dot(normed2, grad_up, 0, 0).astype(bf16)
    grad_norm2 = lax.psum_scatter(dot(grad_up, wu, 1, 1).astype(bf16), tp, scatter_dimension=0, tiled=True).astype(f32)
    mid_norm, g_gain2, g_bias2 = norm_back(n2, inv2, vecs[2], grad_norm2)
    grad_middle = cotangent[0].astype(f32) + mid_norm
    grad_proj = lax.all_gather(grad_middle.astype(bf16), tp, axis=0, tiled=True)
    g_out = dot(attn_out, grad_proj, 0, 0).astype(bf16)
    grad_attn = dot(grad_proj, wo, 1, 1).astype(bf16)
    grad_qkv = attn_bwd(lens, qkv, grad_attn, lse)
    g_qkv = dot(normed1, grad_qkv, 0, 0).astype(bf16)
    grad_norm1 = lax.psum_scatter(dot(grad_qkv, wq, 1, 1).astype(bf16), tp, scatter_dimension=0, tiled=True).astype(f32)
    in_norm, g_gain1, g_bias1 = norm_back(n1, inv1, vecs[0], grad_norm1)
    grad_inputs = grad_middle + in_norm

    def owned_rows(g):
        return lax.psum_scatter(g, "fsdp", scatter_dimension=0, tiled=True)

    def owned_cols(g, groups):
        g = lax.psum_scatter(g.reshape(dpn, width // dpn, -1), "fsdp", scatter_dimension=1, tiled=True)
        g = lax.all_to_all(g, tp, 0, 0, tiled=True)
        g = g.reshape(dpn, rows, groups, -1).transpose(1, 2, 0, 3)
        return g.reshape(rows, -1).astype(f32)

    o_down = owned_rows(g_down).astype(f32)
    o_up = owned_cols(g_up, 1)
    o_out = owned_rows(g_out).astype(f32)
    o_qkv = owned_cols(g_qkv, 3)
    small = jnp.stack([g_gain1, g_bias1, g_gain2, g_bias2]).reshape(4, dpn * fsn, rows).transpose(1, 0, 2)
    small = lax.psum_scatter(small.reshape(dpn * fsn, 4 * rows), ("dp", "fsdp"), scatter_dimension=0, tiled=True).reshape(4, rows)
    return (result[None], grad_inputs[None], o_qkv, o_out, o_up, o_down, small[0], small[1], small[2], small[3])


def solution(mesh):
    split = P(("dp", "fsdp"), None)
    vec = P(("dp", "fsdp"))
    acts = P("fsdp", "dp", None)
    return jax.shard_map(
        on_device,
        mesh=mesh,
        in_specs=(acts, acts, P(), P(), P("fsdp"), split, split, split, split, vec, vec, vec, vec),
        out_specs=(acts, acts, split, split, split, split, vec, vec, vec, vec),
        check_vma=False,
    )
```

```python
import functools

import jax
import jax.numpy as jnp
from jax import lax
from jax.experimental import pallas as pl
from jax.experimental.pallas import tpu as pltpu
from jax.sharding import PartitionSpec as P

HEAD_DIM = 64
EPS = 1e-05
MASKED = -1e30
BLOCK = 256

f32 = jnp.float32
bf16 = jnp.bfloat16


def dot(a, b, ca, cb):
    return lax.dot_general(a, b, (((ca,), (cb,)), ((), ())), preferred_element_type=f32)


def row_limit(start, rows, phon, acou):
    pos = start + lax.broadcasted_iota(jnp.int32, (1, rows), 1)
    return jnp.where(pos < phon + acou, jnp.maximum(pos, phon - 1), phon - 1)


def head_mask(width, head):
    lane = lax.broadcasted_iota(jnp.int32, (1, width), 1)
    return (lane >= head * HEAD_DIM) & (lane < (head + 1) * HEAD_DIM)


def attn_fwd_kernel(lens, qkv, out, lse):
    width = out.shape[1]
    heads = width // HEAD_DIM
    length = out.shape[0]
    phon, acou = lens[0], lens[1]
    scale = HEAD_DIM ** (-0.5)
    for start in range(0, length, BLOCK):
        seen = start + BLOCK
        q = qkv[start : start + BLOCK, :width] * scale
        k = qkv[:seen, width : 2 * width]
        v = qkv[:seen, 2 * width :]
        limit = row_limit(start, BLOCK, phon, acou)
        key = lax.broadcasted_iota(jnp.int32, (seen, 1), 0)
        hidden = key > limit
        total = jnp.zeros((BLOCK, width), f32)
        rows = []
        for h in range(heads):
            mine = head_mask(width, h)
            qh = jnp.where(mine, q, 0)
            s = dot(k, qh, 1, 1)
            s = jnp.where(hidden, MASKED, s)
            top = jnp.max(s, axis=0, keepdims=True)
            e = jnp.exp(s - top)
            tot = jnp.sum(e, axis=0, keepdims=True)
            p = (e * (1.0 / tot)).astype(bf16)
            o = dot(p, v, 0, 0)
            total = total + jnp.where(mine, o, 0)
            rows.append(top + jnp.log(tot))
        out[start : start + BLOCK, :] = total.astype(bf16)
        lse[:, start : start + BLOCK] = jnp.concatenate(rows + [jnp.zeros((8 - heads, BLOCK), f32)], axis=0)


def attn_bwd_kernel(lens, qkv, grad, lse, dqkv, dk_acc, dv_acc):
    width = grad.shape[1]
    heads = width // HEAD_DIM
    length = grad.shape[0]
    phon, acou = lens[0], lens[1]
    scale = HEAD_DIM ** (-0.5)
    for start in reversed(range(0, length, BLOCK)):
        seen = start + BLOCK
        q = qkv[start : start + BLOCK, :width] * scale
        g = grad[start : start + BLOCK, :]
        k = qkv[:seen, width : 2 * width]
        v = qkv[:seen, 2 * width :]
        limit = row_limit(start, BLOCK, phon, acou)
        key = lax.broadcasted_iota(jnp.int32, (seen, 1), 0)
        hidden = key > limit
        dq = jnp.zeros((BLOCK, width), f32)
        for h in range(heads):
            mine = head_mask(width, h)
            qh = jnp.where(mine, q, 0)
            gh = jnp.where(mine, g, 0)
            s = dot(k, qh, 1, 1)
            s = jnp.where(hidden, MASKED, s)
            p = jnp.exp(s - lse[h : h + 1, start : start + BLOCK])
            gp = dot(v, gh, 1, 1)
            delta = jnp.sum(p * gp, axis=0, keepdims=True)
            ds = (p * (gp - delta)).astype(bf16)
            dvh = dot(p.astype(bf16), gh, 1, 0)
            dkh = dot(ds, qh, 1, 0)
            if start == length - BLOCK and h == 0:
                dv_acc[...] = dvh
                dk_acc[...] = dkh
            else:
                dv_acc[:seen, :] += dvh
                dk_acc[:seen, :] += dkh
            dq = dq + jnp.where(mine, dot(ds, k, 0, 0), 0)
        dqkv[start : start + BLOCK, :width] = (dq * scale).astype(bf16)
    dqkv[:, width : 2 * width] = dk_acc[...].astype(bf16)
    dqkv[:, 2 * width :] = dv_acc[...].astype(bf16)


VMEM = pl.BlockSpec(memory_space=pltpu.VMEM)
SMEM = pl.BlockSpec(memory_space=pltpu.SMEM)


def attn_fwd(lens, qkv):
    length, width = qkv.shape[0], qkv.shape[1] // 3
    return pl.pallas_call(
        attn_fwd_kernel,
        out_shape=(jax.ShapeDtypeStruct((length, width), bf16), jax.ShapeDtypeStruct((8, length), f32)),
        in_specs=[SMEM, VMEM],
        out_specs=(VMEM, VMEM),
        compiler_params=pltpu.CompilerParams(vmem_limit_bytes=40 * 2**20),
        cost_estimate=pl.CostEstimate(flops=4 * length * length * width, bytes_accessed=8 * length * width, transcendentals=length * length * width // HEAD_DIM),
        name="attn_fwd",
    )(lens, qkv)


def attn_bwd(lens, qkv, grad, lse):
    length, width = grad.shape
    return pl.pallas_call(
        attn_bwd_kernel,
        out_shape=jax.ShapeDtypeStruct((length, 3 * width), bf16),
        in_specs=[SMEM, VMEM, VMEM, VMEM],
        out_specs=VMEM,
        scratch_shapes=[pltpu.VMEM((length, width), f32), pltpu.VMEM((length, width), f32)],
        compiler_params=pltpu.CompilerParams(vmem_limit_bytes=40 * 2**20),
        cost_estimate=pl.CostEstimate(flops=10 * length * length * width, bytes_accessed=14 * length * width, transcendentals=length * length * width // HEAD_DIM),
        name="attn_bwd",
    )(lens, qkv, grad, lse)


def norm_parts(v):
    mean = jnp.mean(v, axis=-1, keepdims=True)
    centered = v - mean
    var = jnp.mean(centered * centered, axis=-1, keepdims=True)
    inv = lax.rsqrt(var + EPS)
    return centered * inv, inv


def norm_back(n, inv, gain, grad):
    g = grad * gain
    dx = inv * (g - jnp.mean(g, axis=-1, keepdims=True) - n * jnp.mean(g * n, axis=-1, keepdims=True))
    return dx, jnp.sum(grad * n, axis=0), jnp.sum(grad, axis=0)


def with_collectives(frames, cotangent, phon_len, acou_len, row_item, w_qkv, w_out, w_up, w_down, ln1_gain, ln1_bias, ln2_gain, ln2_bias):
    tp, dpn, fsn = "dp", lax.axis_size("dp"), lax.axis_size("fsdp")
    width = frames.shape[2]
    part = width // dpn
    rows = w_up.shape[0]

    vecs = jnp.concatenate([ln1_gain, ln1_bias, ln2_gain, ln2_bias])[None]
    vecs = lax.all_gather(vecs, ("dp", "fsdp"), axis=0, tiled=True)
    vecs = vecs.reshape(dpn * fsn, 4, rows).transpose(1, 0, 2).reshape(4, width).astype(f32)

    qkv_cols = w_qkv.reshape(rows, 3, dpn, part).transpose(2, 0, 1, 3).reshape(dpn, rows, 3 * part)
    qkv_cols = lax.all_to_all(qkv_cols, tp, 0, 0, tiled=True)
    wq = lax.all_gather(qkv_cols, "fsdp", axis=1, tiled=True).reshape(width, 3 * part)
    wo = lax.all_gather(w_out, "fsdp", axis=0, tiled=True)
    ff = w_up.shape[1] // dpn
    up_cols = w_up.reshape(rows, dpn, ff).transpose(1, 0, 2)
    up_cols = lax.all_to_all(up_cols, tp, 0, 0, tiled=True)
    wu = lax.all_gather(up_cols, "fsdp", axis=1, tiled=True).reshape(width, ff)
    wd = lax.all_gather(w_down, "fsdp", axis=0, tiled=True)

    item = row_item[0]
    pick = jnp.arange(phon_len.shape[0], dtype=jnp.int32) == item
    lens = jnp.stack([jnp.sum(jnp.where(pick, phon_len, 0)), jnp.sum(jnp.where(pick, acou_len, 0))])

    x = frames[0].astype(f32)
    n1, inv1 = norm_parts(x)
    normed1 = lax.all_gather((n1 * vecs[0] + vecs[1]).astype(bf16), tp, axis=0, tiled=True)
    grad_down = lax.all_gather(cotangent[0], tp, axis=0, tiled=True)
    qkv = jnp.dot(normed1, wq, preferred_element_type=f32).astype(bf16)
    attn_out, lse = attn_fwd(lens, qkv)
    proj = jnp.dot(attn_out, wo, preferred_element_type=f32).astype(bf16)
    middle = x + lax.psum_scatter(proj, tp, scatter_dimension=0, tiled=True).astype(f32)
    n2, inv2 = norm_parts(middle)
    normed2 = lax.all_gather((n2 * vecs[2] + vecs[3]).astype(bf16), tp, axis=0, tiled=True)
    up_out = jnp.dot(normed2, wu, preferred_element_type=f32)
    cdf = 0.5 * (1.0 + lax.erf(up_out * (0.5**0.5)))
    act_out = (up_out * cdf).astype(bf16)
    down = jnp.dot(act_out, wd, preferred_element_type=f32).astype(bf16)
    result = (middle + lax.psum_scatter(down, tp, scatter_dimension=0, tiled=True).astype(f32)).astype(bf16)

    g_down = dot(act_out, grad_down, 0, 0).astype(bf16)
    slope = cdf + up_out * (jnp.exp(-0.5 * up_out * up_out) * (1.0 / (2.0 * jnp.pi) ** 0.5))
    grad_up = (dot(grad_down, wd, 1, 1) * slope).astype(bf16)
    g_up = dot(normed2, grad_up, 0, 0).astype(bf16)
    grad_norm2 = lax.psum_scatter(dot(grad_up, wu, 1, 1).astype(bf16), tp, scatter_dimension=0, tiled=True).astype(f32)
    mid_norm, g_gain2, g_bias2 = norm_back(n2, inv2, vecs[2], grad_norm2)
    grad_middle = cotangent[0].astype(f32) + mid_norm
    grad_proj = lax.all_gather(grad_middle.astype(bf16), tp, axis=0, tiled=True)
    g_out = dot(attn_out, grad_proj, 0, 0).astype(bf16)
    grad_attn = dot(grad_proj, wo, 1, 1).astype(bf16)
    grad_qkv = attn_bwd(lens, qkv, grad_attn, lse)
    g_qkv = dot(normed1, grad_qkv, 0, 0).astype(bf16)
    grad_norm1 = lax.psum_scatter(dot(grad_qkv, wq, 1, 1).astype(bf16), tp, scatter_dimension=0, tiled=True).astype(f32)
    in_norm, g_gain1, g_bias1 = norm_back(n1, inv1, vecs[0], grad_norm1)
    grad_inputs = grad_middle + in_norm

    def owned_rows(g):
        return lax.psum_scatter(g, "fsdp", scatter_dimension=0, tiled=True)

    def owned_cols(g, groups):
        g = lax.psum_scatter(g.reshape(dpn, width // dpn, -1), "fsdp", scatter_dimension=1, tiled=True)
        g = lax.all_to_all(g, tp, 0, 0, tiled=True)
        g = g.reshape(dpn, rows, groups, -1).transpose(1, 2, 0, 3)
        return g.reshape(rows, -1).astype(f32)

    o_down = owned_rows(g_down).astype(f32)
    o_up = owned_cols(g_up, 1)
    o_out = owned_rows(g_out).astype(f32)
    o_qkv = owned_cols(g_qkv, 3)
    small = jnp.stack([g_gain1, g_bias1, g_gain2, g_bias2]).reshape(4, dpn * fsn, rows).transpose(1, 0, 2)
    small = lax.psum_scatter(small.reshape(dpn * fsn, 4 * rows), ("dp", "fsdp"), scatter_dimension=0, tiled=True).reshape(4, rows)
    return (result[None], grad_inputs[None], o_qkv, o_out, o_up, o_down, small[0], small[1], small[2], small[3])


CHUNKS = 2
SENDS = 320
ARRIVALS = 320
MESH = pl.DeviceIdType.MESH


def layer_kernel(
    lens, frames, cot, vec_in, wq_in, wo_in, wu_in, wd_in,
    o_res, o_in, o_q, o_o, o_u, o_d, o_small,
    VG, VEC, WQ, WO, WU, WD, N1F, INV1, N1, COT, QKV, ATT, LSE, PA, PB,
    LA1, LA2, LB1, LB2, LC1, LC2, LD1, LD2,
    MID, N2F, INV2, NORM2, ACT, SLOPE, GUP, GPROJ, GATT, GQKV, DK, DV,
    GD, GU, GO, GQ, YD, YU, YO, YQ, SU, SQ, ZD, ZU, ZO, ZQ, TU, TQ, RU, RQ,
    SM, SM1, SM2, SM3, SM4, SM5,
    ssem, rsem,
):
    dpn, fsn = lax.axis_size("dp"), lax.axis_size("fsdp")
    nz = fsn // 2
    width = frames.shape[1]
    own = frames.shape[0]
    part = width // dpn
    rows = wu_in.shape[1]
    d, f = lax.axis_index("dp"), lax.axis_index("fsdp")
    c, x = lax.rem(d, 2), lax.div(d, 2)
    y, z = lax.rem(f, 2), lax.div(f, 2)
    core = d + 1 - 2 * c
    far = lax.rem(d + 2, dpn)
    other = lax.rem(core + 2, dpn)
    order = (d, core, far, other)
    pair = (d, f + 1 - 2 * y)
    count = {"send": 0, "arrive": 0}
    sent = []

    def slots(n):
        base = count["arrive"]
        count["arrive"] += n
        assert count["arrive"] <= ARRIVALS
        return base

    def push(src, dst, slot, device):
        i = count["send"]
        count["send"] += 1
        assert i < SENDS
        copy = pltpu.make_async_remote_copy(src, dst, ssem.at[i], rsem.at[slot], device_id=device, device_id_type=MESH)
        copy.start()
        sent.append(copy)
        return copy

    def arrive(ref, slot):
        pltpu.make_async_remote_copy(ref, ref, ssem.at[0], rsem.at[slot], device_id=pair, device_id_type=MESH).wait_recv()

    def zpeer(k):
        return lax.rem(z + k, nz)

    barrier = pltpu.get_barrier_semaphore()
    peers = [(lax.rem(d + k, dpn), f) for k in range(1, dpn)] + [(d, lax.rem(f + k, fsn)) for k in range(1, fsn)]
    for device in peers:
        pl.semaphore_signal(barrier, inc=1, device_id=device, device_id_type=MESH)
    pl.semaphore_wait(barrier, len(peers))

    vec_f, vec_d = slots(fsn), slots(dpn)
    for k in range(1, fsn):
        push(vec_in, VG.at[d, f], vec_f + f, (d, lax.rem(f + k, fsn)))
    mix_q, mix_u = slots(dpn), slots(dpn)
    for k in range(1, dpn):
        dd = lax.rem(d + k, dpn)
        push(wq_in.at[dd], WQ.at[d, f], mix_q + d, (dd, f))
    for k in range(1, dpn):
        dd = lax.rem(d + k, dpn)
        push(wu_in.at[dd], WU.at[d, f], mix_u + d, (dd, f))
    zq, zo, zu, zd = slots(nz), slots(nz), slots(nz), slots(nz)
    yq, yo, yu, yd = slots(nz), slots(nz), slots(nz), slots(nz)
    VG[d, f] = vec_in[...]
    WQ[d, f] = wq_in[d]
    WU[d, f] = wu_in[d]
    WO[f] = wo_in[...]
    WD[f] = wd_in[...]

    def norm_rows(v, nf, inv):
        n, i = norm_parts(v)
        nf[...] = n
        inv[...] = i

    norm_rows(frames[...].astype(f32), N1F, INV1)
    for k in range(1, fsn):
        s = lax.rem(f + k, fsn)
        arrive(VG.at[d, s], vec_f + s)
    for k in range(1, dpn):
        push(VG.at[d], VG.at[d], vec_d + d, (lax.rem(d + k, dpn), f))

    def along(ref_at, zs):
        for k in range(1, nz):
            push(ref_at(f), ref_at(f), zs + z, (d, zpeer(k) * 2 + y))

    def across_own(ref_at, ys):
        push(ref_at(f), ref_at(f), ys + z, pair)

    def forward(ref_at, zs, ys):
        for k in range(1, nz):
            zz = zpeer(k)
            ref = ref_at(zz * 2 + y)
            arrive(ref, zs + zz)
            push(ref, ref, ys + zz, pair)

    def gathered(ref_at, ys):
        for zz in range(nz):
            arrive(ref_at(2 * zz + 1 - y), ys + zz)

    def q_at(s):
        return WQ.at[:, s]

    def o_at(s):
        return WO.at[s]

    def u_at(s):
        return WU.at[:, s]

    def d_at(s):
        return WD.at[s]

    for k in range(1, dpn):
        s = lax.rem(d + k, dpn)
        arrive(WQ.at[s, f], mix_q + s)
    along(q_at, zq)
    across_own(q_at, yq)
    along(o_at, zo)
    for k in range(1, dpn):
        s = lax.rem(d + k, dpn)
        arrive(WU.at[s, f], mix_u + s)
    along(u_at, zu)
    along(d_at, zd)
    for k in range(1, dpn):
        s = lax.rem(d + k, dpn)
        arrive(VG.at[s], vec_d + s)
    group = 128 // rows
    for m in range(width // 128):
        total = VG[(m * group) // fsn, (m * group) % fsn]
        for j in range(1, group):
            total = total + VG[(m * group + j) // fsn, (m * group + j) % fsn]
        VEC[:, m * 128 : (m + 1) * 128] = total

    step = own // CHUNKS

    def ag_start(ref, base):
        for device in (far, core):
            for h in range(CHUNKS):
                piece = ref.at[d, h * step : (h + 1) * step]
                push(piece, piece, base + d * CHUNKS + h, (device, f))

    def ag_forward(ref, base):
        for h in range(CHUNKS):
            piece = ref.at[far, h * step : (h + 1) * step]
            arrive(piece, base + far * CHUNKS + h)
            push(piece, piece, base + far * CHUNKS + h, (core, f))

    def ag_wait(ref, base, b):
        for h in range(CHUNKS):
            arrive(ref.at[b, h * step : (h + 1) * step], base + b * CHUNKS + h)

    def rs_send(P, L1, L2, base, compute):
        for j, hi in enumerate((1 - x, x)):
            b_send, b_keep = hi * 2 + 1 - c, hi * 2 + c
            compute(b_send)
            push(P.at[b_send], L1.at[j], base + j, (core, f))
            if j == 0:
                compute(b_keep)
        b_far = (1 - x) * 2 + c
        arrive(L1.at[0], base)
        P[b_far] = (P[b_far].astype(f32) + L1[0].astype(f32)).astype(bf16)
        push(P.at[b_far], L2, base + 2, (far, f))
        compute(d)

    def rs_total(P, L1, L2, base):
        arrive(L1.at[1], base + 1)
        arrive(L2, base + 2)
        return P[d].astype(f32) + L1[1].astype(f32) + L2[...].astype(f32)

    def lines(b):
        return pl.ds(pl.multiple_of(b * own, own), own)

    def tile(i):
        return slice(i * part, (i + 1) * part)

    ag1, agc, ag2, agp = slots(dpn * CHUNKS), slots(dpn * CHUNKS), slots(dpn * CHUNKS), slots(dpn * CHUNKS)
    rs1, rs2, rs3, rs4 = slots(3), slots(3), slots(3), slots(3)

    N1[d] = (N1F[...] * VEC[0:1, :] + VEC[1:2, :]).astype(bf16)
    COT[d] = cot[...]
    ag_start(N1, ag1)
    forward(q_at, zq, yq)
    across_own(o_at, yo)
    across_own(u_at, yu)
    across_own(d_at, yd)
    ag_forward(N1, ag1)
    ag_start(COT, agc)
    gathered(q_at, yq)
    for n, b in enumerate(order):
        if n in (1, 3):
            ag_wait(N1, ag1, b)
        QKV[lines(b), :] = dot(N1[b], WQ[...].reshape(width, 3 * part), 1, 0).astype(bf16)
    forward(o_at, zo, yo)
    attn_fwd_kernel(lens, QKV, ATT, LSE)
    ag_forward(COT, agc)
    gathered(o_at, yo)

    def proj(b):
        PA[b] = dot(ATT[lines(b), :], WO[...].reshape(part, width), 1, 0).astype(bf16)

    proj_sends = len(sent)
    rs_send(PA, LA1, LA2, rs1, proj)
    proj_sends = sent[proj_sends:]
    forward(u_at, zu, yu)
    MID[...] = frames[...].astype(f32) + rs_total(PA, LA1, LA2, rs1)
    norm_rows(MID[...], N2F, INV2)
    NORM2[d] = (N2F[...] * VEC[2:3, :] + VEC[3:4, :]).astype(bf16)
    ag_start(NORM2, ag2)
    gathered(u_at, yu)

    def up(b):
        for i in range(dpn):
            u = dot(NORM2[b], WU[:, :, :, tile(i)].reshape(width, part), 1, 0)
            cdf = 0.5 * (1.0 + lax.erf(u * (0.5**0.5)))
            ACT[b, :, tile(i)] = (u * cdf).astype(bf16)
            SLOPE[b, :, tile(i)] = cdf + u * (jnp.exp(-0.5 * u * u) * (1.0 / (2.0 * jnp.pi) ** 0.5))

    up(d)
    ag_wait(NORM2, ag2, core)
    up(core)
    ag_forward(NORM2, ag2)
    up(far)
    ag_wait(NORM2, ag2, other)
    up(other)
    forward(d_at, zd, yd)
    ag_wait(COT, agc, core)
    ag_wait(COT, agc, other)
    gathered(d_at, yd)
    per = fsn // dpn

    def grad_hidden(b):
        for i in range(dpn):
            g = dot(COT[b], WD[i * per : (i + 1) * per].reshape(part, width), 1, 1)
            GUP[b, :, tile(i)] = (g * SLOPE[b, :, tile(i)]).astype(bf16)
        for i in range(dpn):
            PB[b, :, tile(i)] = dot(GUP[b], WU[i].reshape(part, width), 1, 1).astype(bf16)

    norm2_sends = len(sent)
    rs_send(PB, LB1, LB2, rs2, grad_hidden)
    norm2_sends = sent[norm2_sends:]

    y_d, y_u, y_o, y_q = slots(nz), slots(dpn), slots(1), slots(dpn)
    z_d, z_u, z_o, z_q = slots(nz), slots(nz), slots(nz), slots(nz)
    big = wd_in.shape[0]
    pairs = part // (2 * big)

    def against(a, b, i):
        return dot(a[:, :, tile(i)].reshape(dpn * own, part), b, 0, 0).astype(bf16)

    for i in range(dpn):
        g = against(ACT, COT[...].reshape(dpn * own, width), i)
        GD[i * pairs : (i + 1) * pairs] = g.reshape(pairs, 2, big, width)
        for j in range(i * pairs, (i + 1) * pairs):
            push(GD.at[j, 1 - y], YD.at[j], y_d + j, pair)

    MIDG = N2F
    grad2 = rs_total(PB, LB1, LB2, rs2)
    mid_norm, gain2, bias2 = norm_back(N2F[...], INV2[...], VEC[2:3, :], grad2)
    MIDG[...] = cot[...].astype(f32) + mid_norm
    GPROJ[d] = MIDG[...].astype(bf16)
    ag_start(GPROJ, agp)

    for copy in proj_sends:
        copy.wait_send()

    for i in range(dpn):
        g = against(NORM2, GUP[...].reshape(dpn * own, width), i)
        GU[i] = g.reshape(nz, 2, rows, width)
        push(GU.at[i, :, 1 - y], YU.at[i], y_u + i, pair)

    def grad_heads(b):
        GATT[lines(b), :] = dot(GPROJ[b], WO[...].reshape(part, width), 1, 1).astype(bf16)

    grad_heads(d)
    ag_forward(GPROJ, agp)
    grad_heads(far)
    ag_wait(GPROJ, agp, core)
    grad_heads(core)
    ag_wait(GPROJ, agp, other)
    grad_heads(other)

    g = dot(ATT[...], GPROJ[...].reshape(dpn * own, width), 0, 0).astype(bf16)
    GO[...] = g.reshape(nz, 2, rows, width)
    push(GO.at[:, 1 - y], YO, y_o, pair)

    def add(a, b):
        return (a.astype(f32) + b.astype(f32)).astype(bf16)

    for j in range(nz):
        arrive(YD.at[j], y_d + j)
        YD[j] = add(GD[j, y], YD[j])
    for k in range(1, nz):
        zz = zpeer(k)
        push(YD.at[zz], ZD.at[z], z_d + z, (d, zz * 2 + y))

    attn_bwd_kernel(lens, QKV, GATT, LSE, GQKV, DK, DV)

    for i in range(dpn):
        arrive(YU.at[i], y_u + i)
        SU[:, i] = add(GU[i, :, y], YU[i])
    for k in range(1, nz):
        zz = zpeer(k)
        push(SU.at[zz], ZU.at[z], z_u + z, (d, zz * 2 + y))

    for i in range(dpn):
        g = against(N1, GQKV[...], i)
        GQ[i] = g.reshape(nz, 2, rows, 3 * part)
        push(GQ.at[i, :, 1 - y], YQ.at[i], y_q + i, pair)

    for copy in norm2_sends:
        copy.wait_send()

    def grad_first(b):
        for i in range(dpn):
            PB[b, :, tile(i)] = dot(GQKV[lines(b), :], WQ[i].reshape(part, 3 * part), 1, 1).astype(bf16)

    rs_send(PB, LD1, LD2, rs4, grad_first)

    arrive(YO, y_o)
    YO[...] = add(GO[:, y], YO[...])
    for k in range(1, nz):
        zz = zpeer(k)
        push(YO.at[zz], ZO.at[z], z_o + z, (d, zz * 2 + y))
    for i in range(dpn):
        arrive(YQ.at[i], y_q + i)
        SQ[:, i] = add(GQ[i, :, y], YQ[i])
    for k in range(1, nz):
        zz = zpeer(k)
        push(SQ.at[zz], ZQ.at[z], z_q + z, (d, zz * 2 + y))

    def down(b):
        PA[b] = dot(ACT[b], WD[...].reshape(width, width), 1, 0).astype(bf16)

    rs_send(PA, LC1, LC2, rs3, down)

    SD, SO = YD, YO

    def settle(S, Z, zs):
        total = S[z].astype(f32)
        for k in range(1, nz):
            zz = zpeer(k)
            arrive(Z.at[zz], zs + zz)
            total = total + Z[zz].astype(f32)
        return total

    back_u, back_q = slots(dpn), slots(dpn)
    TU[...] = settle(SU, ZU, z_u).astype(bf16)
    for k in range(1, dpn):
        dd = lax.rem(d + k, dpn)
        push(TU.at[dd], RU.at[d], back_u + d, (dd, f))
    RU[d] = TU[d]

    grad1 = rs_total(PB, LD1, LD2, rs4)
    in_norm, gain1, bias1 = norm_back(N1F[...], INV1[...], VEC[0:1, :], grad1)
    o_in[...] = MIDG[...] + in_norm
    small = jnp.concatenate([v.reshape(1, width) for v in (gain1, bias1, gain2, bias2)] + [jnp.zeros((4, width), f32)], axis=0)
    for i in range(dpn):
        SM[i] = small[:, tile(i)]
    sm_d, sm_y, sm_z = slots(dpn), slots(1), slots(nz)
    for k in range(1, dpn):
        dd = lax.rem(d + k, dpn)
        push(SM.at[dd], SM1.at[d], sm_d + d, (dd, f))

    o_d[...] = settle(SD, ZD, z_d)
    o_o[...] = settle(SO, ZO, z_o)

    total = SM[d]
    for k in range(1, dpn):
        s = lax.rem(d + k, dpn)
        arrive(SM1.at[s], sm_d + s)
        total = total + SM1[s]
    SM2[...] = total
    push(SM2, SM3, sm_y, pair)

    TQ[...] = settle(SQ, ZQ, z_q).astype(bf16)
    for k in range(1, dpn):
        dd = lax.rem(d + k, dpn)
        push(TQ.at[dd], RQ.at[d], back_q + d, (dd, f))
    RQ[d] = TQ[d]

    arrive(SM3, sm_y)
    SM4[...] = SM2[...] + SM3[...]
    for k in range(1, nz):
        push(SM4, SM5.at[z], sm_z + z, (d, zpeer(k) * 2 + y))

    o_res[...] = (MID[...] + rs_total(PA, LC1, LC2, rs3)).astype(bf16)
    for k in range(1, dpn):
        s = lax.rem(d + k, dpn)
        arrive(RU.at[s], back_u + s)
    for s in range(dpn):
        o_u[:, s * width : (s + 1) * width] = RU[s].astype(f32)
    for k in range(1, dpn):
        s = lax.rem(d + k, dpn)
        arrive(RQ.at[s], back_q + s)
    for s in range(dpn):
        for j in range(3):
            o_q[:, j * width + s * part : j * width + (s + 1) * part] = RQ[s, :, tile(j)].astype(f32)
    total = SM4[...]
    for k in range(1, nz):
        zz = zpeer(k)
        arrive(SM5.at[zz], sm_z + zz)
        total = total + SM5[zz]
    o_small[...] = total

    waited = set(map(id, proj_sends + norm2_sends))
    for copy in sent:
        if id(copy) not in waited:
            copy.wait_send()


def in_one_kernel(frames, cotangent, phon_len, acou_len, row_item, w_qkv, w_out, w_up, w_down, ln1_gain, ln1_bias, ln2_gain, ln2_bias):
    dpn, fsn = lax.axis_size("dp"), lax.axis_size("fsdp")
    nz = fsn // 2
    own, width = frames.shape[1:]
    length = dpn * own
    part = width // dpn
    rows = w_up.shape[0]
    big = w_down.shape[0]
    item = row_item[0]
    pick = jnp.arange(phon_len.shape[0], dtype=jnp.int32) == item
    lens = jnp.stack([jnp.sum(jnp.where(pick, phon_len, 0)), jnp.sum(jnp.where(pick, acou_len, 0))])
    place = lax.axis_index("fsdp") * rows % 128
    vec = jnp.stack([ln1_gain, ln1_bias, ln2_gain, ln2_bias]).astype(f32)
    vec = jnp.pad(vec, ((0, 4), (0, 128 - rows)))
    vec = jnp.roll(vec, place, axis=1)
    wq = w_qkv.reshape(rows, 3, dpn, part).transpose(2, 0, 1, 3).reshape(dpn, rows, 3 * part)
    wu = w_up.reshape(rows, dpn, width).transpose(1, 0, 2)

    def buf(*shape, dtype=bf16):
        return pltpu.VMEM(shape, dtype)

    full = buf(dpn, own, width)
    land = [buf(2, own, width), buf(own, width)]
    scratch = [
        buf(dpn, fsn, 8, 128, dtype=f32), buf(8, width, dtype=f32),
        buf(dpn, fsn, rows, 3 * part), buf(fsn, rows, width), buf(dpn, fsn, rows, width), buf(fsn, big, width),
        buf(own, width, dtype=f32), buf(own, 1, dtype=f32), full, full,
        buf(length, 3 * part), buf(length, part), buf(8, length, dtype=f32), full, full,
        *land, *land, *land, *land,
        buf(own, width, dtype=f32), buf(own, width, dtype=f32), buf(own, 1, dtype=f32),
        full, full, buf(dpn, own, width, dtype=f32), full, full,
        buf(length, part), buf(length, 3 * part), buf(length, part, dtype=f32), buf(length, part, dtype=f32),
        buf(nz, 2, big, width), buf(dpn, nz, 2, rows, width), buf(nz, 2, rows, width), buf(dpn, nz, 2, rows, 3 * part),
        buf(nz, big, width), buf(dpn, nz, rows, width), buf(nz, rows, width), buf(dpn, nz, rows, 3 * part),
        buf(nz, dpn, rows, width), buf(nz, dpn, rows, 3 * part),
        buf(nz, big, width), buf(nz, dpn, rows, width), buf(nz, rows, width), buf(nz, dpn, rows, 3 * part),
        buf(dpn, rows, width), buf(dpn, rows, 3 * part), buf(dpn, rows, width), buf(dpn, rows, 3 * part),
        buf(dpn, 8, part, dtype=f32), buf(dpn, 8, part, dtype=f32), buf(8, part, dtype=f32), buf(8, part, dtype=f32),
        buf(8, part, dtype=f32), buf(nz, 8, part, dtype=f32),
        pltpu.SemaphoreType.DMA((SENDS,)), pltpu.SemaphoreType.DMA((ARRIVALS,)),
    ]
    outs = pl.pallas_call(
        layer_kernel,
        out_shape=(
            jax.ShapeDtypeStruct((own, width), bf16),
            jax.ShapeDtypeStruct((own, width), f32),
            jax.ShapeDtypeStruct((rows, 3 * width), f32),
            jax.ShapeDtypeStruct((rows, width), f32),
            jax.ShapeDtypeStruct((rows, dpn * width), f32),
            jax.ShapeDtypeStruct((big, width), f32),
            jax.ShapeDtypeStruct((8, part), f32),
        ),
        in_specs=[SMEM] + [VMEM] * 7,
        out_specs=(VMEM,) * 7,
        scratch_shapes=scratch,
        compiler_params=pltpu.CompilerParams(collective_id=0, has_side_effects=True, vmem_limit_bytes=67043328),
        name="layer",
    )(lens, frames[0], cotangent[0], vec, wq, w_out, wu, w_down)
    small = lax.dynamic_slice(outs[6], (0, lax.axis_index("fsdp") * rows), (4, rows))
    return (outs[0][None], outs[1][None], *outs[2:6], small[0], small[1], small[2], small[3])


def on_device(*args):
    dpn, fsn, rows, width = lax.axis_size("dp"), lax.axis_size("fsdp"), args[7].shape[0], args[7].shape[1]
    fits = dpn == 4 and fsn % dpn == 0 and rows % 16 == 0 and 128 % rows == 0
    return (in_one_kernel if fits else with_collectives)(*args)


def solution(mesh):
    split = P(("dp", "fsdp"), None)
    vec = P(("dp", "fsdp"))
    acts = P("fsdp", "dp", None)
    return jax.shard_map(
        on_device,
        mesh=mesh,
        in_specs=(acts, acts, P(), P(), P("fsdp"), split, split, split, split, vec, vec, vec, vec),
        out_specs=(acts, acts, split, split, split, split, vec, vec, vec, vec),
        check_vma=False,
    )
```

```python
import functools

import jax
import jax.numpy as jnp
from jax import lax
from jax.experimental import pallas as pl
from jax.experimental.pallas import tpu as pltpu
from jax.sharding import PartitionSpec as P

HEAD_DIM = 64
EPS = 1e-05
MASKED = -1e30
BLOCK = 256

f32 = jnp.float32
bf16 = jnp.bfloat16


def dot(a, b, ca, cb):
    return lax.dot_general(a, b, (((ca,), (cb,)), ((), ())), preferred_element_type=f32)


def row_limit(start, rows, phon, acou):
    pos = start + lax.broadcasted_iota(jnp.int32, (1, rows), 1)
    return jnp.where(pos < phon + acou, jnp.maximum(pos, phon - 1), phon - 1)


def head_mask(width, head):
    lane = lax.broadcasted_iota(jnp.int32, (1, width), 1)
    return (lane >= head * HEAD_DIM) & (lane < (head + 1) * HEAD_DIM)


def attn_fwd_kernel(lens, qkv, out, lse, between={}):
    width = out.shape[1]
    heads = width // HEAD_DIM
    length = out.shape[0]
    phon, acou = lens[0], lens[1]
    scale = HEAD_DIM ** (-0.5)
    for start in range(0, length, BLOCK):
        if start // BLOCK in between:
            between[start // BLOCK]()
        seen = start + BLOCK
        q = qkv[start : start + BLOCK, :width] * scale
        k = qkv[:seen, width : 2 * width]
        v = qkv[:seen, 2 * width :]
        limit = row_limit(start, BLOCK, phon, acou)
        key = lax.broadcasted_iota(jnp.int32, (seen, 1), 0)
        hidden = key > limit
        total = jnp.zeros((BLOCK, width), f32)
        rows = []
        for h in range(heads):
            mine = head_mask(width, h)
            qh = jnp.where(mine, q, 0)
            s = dot(k, qh, 1, 1)
            s = jnp.where(hidden, MASKED, s)
            top = jnp.max(s, axis=0, keepdims=True)
            e = jnp.exp(s - top)
            tot = jnp.sum(e, axis=0, keepdims=True)
            p = (e * (1.0 / tot)).astype(bf16)
            o = dot(p, v, 0, 0)
            total = total + jnp.where(mine, o, 0)
            rows.append(top + jnp.log(tot))
        out[start : start + BLOCK, :] = total.astype(bf16)
        lse[:, start : start + BLOCK] = jnp.concatenate(rows + [jnp.zeros((8 - heads, BLOCK), f32)], axis=0)


def attn_bwd_kernel(lens, qkv, grad, lse, dqkv, dk_acc, dv_acc, between={}):
    width = grad.shape[1]
    heads = width // HEAD_DIM
    length = grad.shape[0]
    phon, acou = lens[0], lens[1]
    scale = HEAD_DIM ** (-0.5)
    for start in reversed(range(0, length, BLOCK)):
        if start // BLOCK in between:
            between[start // BLOCK]()
        seen = start + BLOCK
        q = qkv[start : start + BLOCK, :width] * scale
        g = grad[start : start + BLOCK, :]
        k = qkv[:seen, width : 2 * width]
        v = qkv[:seen, 2 * width :]
        limit = row_limit(start, BLOCK, phon, acou)
        key = lax.broadcasted_iota(jnp.int32, (seen, 1), 0)
        hidden = key > limit
        dq = jnp.zeros((BLOCK, width), f32)
        for h in range(heads):
            mine = head_mask(width, h)
            qh = jnp.where(mine, q, 0)
            gh = jnp.where(mine, g, 0)
            s = dot(k, qh, 1, 1)
            s = jnp.where(hidden, MASKED, s)
            p = jnp.exp(s - lse[h : h + 1, start : start + BLOCK])
            gp = dot(v, gh, 1, 1)
            delta = jnp.sum(p * gp, axis=0, keepdims=True)
            ds = (p * (gp - delta)).astype(bf16)
            dvh = dot(p.astype(bf16), gh, 1, 0)
            dkh = dot(ds, qh, 1, 0)
            if start == length - BLOCK and h == 0:
                dv_acc[...] = dvh
                dk_acc[...] = dkh
            else:
                dv_acc[:seen, :] += dvh
                dk_acc[:seen, :] += dkh
            dq = dq + jnp.where(mine, dot(ds, k, 0, 0), 0)
        dqkv[start : start + BLOCK, :width] = (dq * scale).astype(bf16)
    dqkv[:, width : 2 * width] = dk_acc[...].astype(bf16)
    dqkv[:, 2 * width :] = dv_acc[...].astype(bf16)


VMEM = pl.BlockSpec(memory_space=pltpu.VMEM)
SMEM = pl.BlockSpec(memory_space=pltpu.SMEM)


def attn_fwd(lens, qkv):
    length, width = qkv.shape[0], qkv.shape[1] // 3
    return pl.pallas_call(
        attn_fwd_kernel,
        out_shape=(jax.ShapeDtypeStruct((length, width), bf16), jax.ShapeDtypeStruct((8, length), f32)),
        in_specs=[SMEM, VMEM],
        out_specs=(VMEM, VMEM),
        compiler_params=pltpu.CompilerParams(vmem_limit_bytes=40 * 2**20),
        cost_estimate=pl.CostEstimate(flops=4 * length * length * width, bytes_accessed=8 * length * width, transcendentals=length * length * width // HEAD_DIM),
        name="attn_fwd",
    )(lens, qkv)


def attn_bwd(lens, qkv, grad, lse):
    length, width = grad.shape
    return pl.pallas_call(
        attn_bwd_kernel,
        out_shape=jax.ShapeDtypeStruct((length, 3 * width), bf16),
        in_specs=[SMEM, VMEM, VMEM, VMEM],
        out_specs=VMEM,
        scratch_shapes=[pltpu.VMEM((length, width), f32), pltpu.VMEM((length, width), f32)],
        compiler_params=pltpu.CompilerParams(vmem_limit_bytes=40 * 2**20),
        cost_estimate=pl.CostEstimate(flops=10 * length * length * width, bytes_accessed=14 * length * width, transcendentals=length * length * width // HEAD_DIM),
        name="attn_bwd",
    )(lens, qkv, grad, lse)


def norm_parts(v):
    mean = jnp.mean(v, axis=-1, keepdims=True)
    centered = v - mean
    var = jnp.mean(centered * centered, axis=-1, keepdims=True)
    inv = lax.rsqrt(var + EPS)
    return centered * inv, inv


def norm_back(n, inv, gain, grad):
    g = grad * gain
    dx = inv * (g - jnp.mean(g, axis=-1, keepdims=True) - n * jnp.mean(g * n, axis=-1, keepdims=True))
    return dx, jnp.sum(grad * n, axis=0), jnp.sum(grad, axis=0)


def with_collectives(frames, cotangent, phon_len, acou_len, row_item, w_qkv, w_out, w_up, w_down, ln1_gain, ln1_bias, ln2_gain, ln2_bias):
    tp, dpn, fsn = "dp", lax.axis_size("dp"), lax.axis_size("fsdp")
    width = frames.shape[2]
    part = width // dpn
    rows = w_up.shape[0]

    vecs = jnp.concatenate([ln1_gain, ln1_bias, ln2_gain, ln2_bias])[None]
    vecs = lax.all_gather(vecs, ("dp", "fsdp"), axis=0, tiled=True)
    vecs = vecs.reshape(dpn * fsn, 4, rows).transpose(1, 0, 2).reshape(4, width).astype(f32)

    qkv_cols = w_qkv.reshape(rows, 3, dpn, part).transpose(2, 0, 1, 3).reshape(dpn, rows, 3 * part)
    qkv_cols = lax.all_to_all(qkv_cols, tp, 0, 0, tiled=True)
    wq = lax.all_gather(qkv_cols, "fsdp", axis=1, tiled=True).reshape(width, 3 * part)
    wo = lax.all_gather(w_out, "fsdp", axis=0, tiled=True)
    ff = w_up.shape[1] // dpn
    up_cols = w_up.reshape(rows, dpn, ff).transpose(1, 0, 2)
    up_cols = lax.all_to_all(up_cols, tp, 0, 0, tiled=True)
    wu = lax.all_gather(up_cols, "fsdp", axis=1, tiled=True).reshape(width, ff)
    wd = lax.all_gather(w_down, "fsdp", axis=0, tiled=True)

    item = row_item[0]
    pick = jnp.arange(phon_len.shape[0], dtype=jnp.int32) == item
    lens = jnp.stack([jnp.sum(jnp.where(pick, phon_len, 0)), jnp.sum(jnp.where(pick, acou_len, 0))])

    x = frames[0].astype(f32)
    n1, inv1 = norm_parts(x)
    normed1 = lax.all_gather((n1 * vecs[0] + vecs[1]).astype(bf16), tp, axis=0, tiled=True)
    grad_down = lax.all_gather(cotangent[0], tp, axis=0, tiled=True)
    qkv = jnp.dot(normed1, wq, preferred_element_type=f32).astype(bf16)
    attn_out, lse = attn_fwd(lens, qkv)
    proj = jnp.dot(attn_out, wo, preferred_element_type=f32).astype(bf16)
    middle = x + lax.psum_scatter(proj, tp, scatter_dimension=0, tiled=True).astype(f32)
    n2, inv2 = norm_parts(middle)
    normed2 = lax.all_gather((n2 * vecs[2] + vecs[3]).astype(bf16), tp, axis=0, tiled=True)
    up_out = jnp.dot(normed2, wu, preferred_element_type=f32)
    cdf = 0.5 * (1.0 + lax.erf(up_out * (0.5**0.5)))
    act_out = (up_out * cdf).astype(bf16)
    down = jnp.dot(act_out, wd, preferred_element_type=f32).astype(bf16)
    result = (middle + lax.psum_scatter(down, tp, scatter_dimension=0, tiled=True).astype(f32)).astype(bf16)

    g_down = dot(act_out, grad_down, 0, 0).astype(bf16)
    slope = cdf + up_out * (jnp.exp(-0.5 * up_out * up_out) * (1.0 / (2.0 * jnp.pi) ** 0.5))
    grad_up = (dot(grad_down, wd, 1, 1) * slope).astype(bf16)
    g_up = dot(normed2, grad_up, 0, 0).astype(bf16)
    grad_norm2 = lax.psum_scatter(dot(grad_up, wu, 1, 1).astype(bf16), tp, scatter_dimension=0, tiled=True).astype(f32)
    mid_norm, g_gain2, g_bias2 = norm_back(n2, inv2, vecs[2], grad_norm2)
    grad_middle = cotangent[0].astype(f32) + mid_norm
    grad_proj = lax.all_gather(grad_middle.astype(bf16), tp, axis=0, tiled=True)
    g_out = dot(attn_out, grad_proj, 0, 0).astype(bf16)
    grad_attn = dot(grad_proj, wo, 1, 1).astype(bf16)
    grad_qkv = attn_bwd(lens, qkv, grad_attn, lse)
    g_qkv = dot(normed1, grad_qkv, 0, 0).astype(bf16)
    grad_norm1 = lax.psum_scatter(dot(grad_qkv, wq, 1, 1).astype(bf16), tp, scatter_dimension=0, tiled=True).astype(f32)
    in_norm, g_gain1, g_bias1 = norm_back(n1, inv1, vecs[0], grad_norm1)
    grad_inputs = grad_middle + in_norm

    def owned_rows(g):
        return lax.psum_scatter(g, "fsdp", scatter_dimension=0, tiled=True)

    def owned_cols(g, groups):
        g = lax.psum_scatter(g.reshape(dpn, width // dpn, -1), "fsdp", scatter_dimension=1, tiled=True)
        g = lax.all_to_all(g, tp, 0, 0, tiled=True)
        g = g.reshape(dpn, rows, groups, -1).transpose(1, 2, 0, 3)
        return g.reshape(rows, -1).astype(f32)

    o_down = owned_rows(g_down).astype(f32)
    o_up = owned_cols(g_up, 1)
    o_out = owned_rows(g_out).astype(f32)
    o_qkv = owned_cols(g_qkv, 3)
    small = jnp.stack([g_gain1, g_bias1, g_gain2, g_bias2]).reshape(4, dpn * fsn, rows).transpose(1, 0, 2)
    small = lax.psum_scatter(small.reshape(dpn * fsn, 4 * rows), ("dp", "fsdp"), scatter_dimension=0, tiled=True).reshape(4, rows)
    return (result[None], grad_inputs[None], o_qkv, o_out, o_up, o_down, small[0], small[1], small[2], small[3])


CHUNKS = 2
SENDS = 320
ARRIVALS = 320
MESH = pl.DeviceIdType.MESH


def layer_kernel(
    lens, frames, cot, vec_in, wq_in, wo_in, wu_in, wd_in,
    o_res, o_in, o_q, o_o, o_u, o_d, o_small,
    VG, VEC, WQ, WO, WU, WD, N1F, INV1, N1, COT, QKV, ATT, LSE, PA, PB,
    LA1, LA2, LB1, LB2, LC1, LC2, LD1, LD2,
    MID, N2F, INV2, NORM2, ACT, SLOPE, GUP, GPROJ, GATT, GQKV, DK, DV,
    GD, GU, GO, GQ, YD, YU, YO, YQ, SU, SQ, ZD, ZU, ZO, ZQ, TU, TQ, RU, RQ,
    SM, SM1, SM2, SM3, SM4, SM5,
    ssem, rsem,
):
    dpn, fsn = lax.axis_size("dp"), lax.axis_size("fsdp")
    nz = fsn // 2
    width = frames.shape[1]
    own = frames.shape[0]
    part = width // dpn
    rows = wu_in.shape[1]
    d, f = lax.axis_index("dp"), lax.axis_index("fsdp")
    c, x = lax.rem(d, 2), lax.div(d, 2)
    y, z = lax.rem(f, 2), lax.div(f, 2)
    core = d + 1 - 2 * c
    far = lax.rem(d + 2, dpn)
    other = lax.rem(core + 2, dpn)
    order = (d, core, far, other)
    pair = (d, f + 1 - 2 * y)
    count = {"send": 0, "arrive": 0}
    sent = []

    def slots(n):
        base = count["arrive"]
        count["arrive"] += n
        assert count["arrive"] <= ARRIVALS
        return base

    def push(src, dst, slot, device, when=None):
        i = count["send"]
        count["send"] += 1
        assert i < SENDS
        copy = pltpu.make_async_remote_copy(src, dst, ssem.at[i], rsem.at[slot], device_id=device, device_id_type=MESH)
        if when is None:
            copy.start()
        else:
            pl.when(when)(lambda: copy.start())
        sent.append((when, copy))

    def sent_out(copies):
        for when, copy in copies:
            if when is None:
                copy.wait_send()
            else:
                pl.when(when)(lambda copy=copy: copy.wait_send())

    def arrive(ref, slot):
        pltpu.make_async_remote_copy(ref, ref, ssem.at[0], rsem.at[slot], device_id=pair, device_id_type=MESH).wait_recv()

    def zpeer(k):
        return lax.rem(z + k, nz)

    barrier = pltpu.get_barrier_semaphore()
    peers = [(lax.rem(d + k, dpn), f) for k in range(1, dpn)] + [(d, lax.rem(f + k, fsn)) for k in range(1, fsn)]
    for device in peers:
        pl.semaphore_signal(barrier, inc=1, device_id=device, device_id_type=MESH)
    pl.semaphore_wait(barrier, len(peers))

    vec_f, vec_d = slots(fsn), slots(dpn)
    for k in range(1, fsn):
        push(vec_in, VG.at[d, f], vec_f + f, (d, lax.rem(f + k, fsn)))
    mix_q, mix_u = slots(dpn), slots(dpn)
    for k in range(1, dpn):
        dd = lax.rem(d + k, dpn)
        push(wq_in.at[dd], WQ.at[d, f], mix_q + d, (dd, f))
    for k in range(1, dpn):
        dd = lax.rem(d + k, dpn)
        push(wu_in.at[dd], WU.at[d, f], mix_u + d, (dd, f))
    zq, zo, zu, zd = slots(nz), slots(nz), slots(nz), slots(nz)
    yq, yo, yu, yd = slots(nz), slots(nz), slots(nz), slots(nz)
    def clip(v):
        return jnp.clip(v, 0, nz - 1)

    def along(ref_at, zs):
        for side in (1, -1):
            to = z + side
            push(ref_at(f), ref_at(f), zs + z, (d, clip(to) * 2 + y), when=(to >= 0) & (to < nz))

    def across_own(ref_at, ys):
        push(ref_at(f), ref_at(f), ys + z, pair)

    def hop(ref_at, zs, ys, h):
        for side in (1, -1):
            src, to = z + side * h, z - side
            here = (src >= 0) & (src < nz)
            ref, src = ref_at(clip(src) * 2 + y), clip(src)
            pl.when(here)(lambda: arrive(ref, zs + src))
            push(ref, ref, zs + src, (d, clip(to) * 2 + y), when=here & (to >= 0) & (to < nz))
            push(ref, ref, ys + src, pair, when=here)

    def forward(ref_at, zs, ys, first=1, last=None):
        for h in range(first, nz if last is None else last + 1):
            hop(ref_at, zs, ys, h)

    def gathered(ref_at, ys):
        for zz in range(nz):
            arrive(ref_at(2 * zz + 1 - y), ys + zz)

    def q_at(s):
        return WQ.at[:, s]

    def o_at(s):
        return WO.at[s]

    def u_at(s):
        return WU.at[:, s]

    def d_at(s):
        return WD.at[s]

    WO[f] = wo_in[...]
    WD[f] = wd_in[...]
    along(o_at, zo)
    across_own(o_at, yo)
    across_own(d_at, yd)
    VG[d, f] = vec_in[...]
    WQ[d, f] = wq_in[d]
    WU[d, f] = wu_in[d]

    def norm_rows(v, nf, inv):
        n, i = norm_parts(v)
        nf[...] = n
        inv[...] = i

    norm_rows(frames[...].astype(f32), N1F, INV1)
    for k in range(1, fsn):
        s = lax.rem(f + k, fsn)
        arrive(VG.at[d, s], vec_f + s)
    for k in range(1, dpn):
        push(VG.at[d], VG.at[d], vec_d + d, (lax.rem(d + k, dpn), f))

    for k in range(1, dpn):
        s = lax.rem(d + k, dpn)
        arrive(WQ.at[s, f], mix_q + s)
    along(q_at, zq)
    across_own(q_at, yq)
    for k in range(1, dpn):
        s = lax.rem(d + k, dpn)
        arrive(WU.at[s, f], mix_u + s)
    along(u_at, zu)
    along(d_at, zd)
    for k in range(1, dpn):
        s = lax.rem(d + k, dpn)
        arrive(VG.at[s], vec_d + s)
    group = 128 // rows
    for m in range(width // 128):
        total = VG[(m * group) // fsn, (m * group) % fsn]
        for j in range(1, group):
            total = total + VG[(m * group + j) // fsn, (m * group + j) % fsn]
        VEC[:, m * 128 : (m + 1) * 128] = total

    step = own // CHUNKS

    def ag_start(ref, base):
        for device in (far, core):
            for h in range(CHUNKS):
                piece = ref.at[d, h * step : (h + 1) * step]
                push(piece, piece, base + d * CHUNKS + h, (device, f))

    def ag_forward(ref, base):
        for h in range(CHUNKS):
            piece = ref.at[far, h * step : (h + 1) * step]
            arrive(piece, base + far * CHUNKS + h)
            push(piece, piece, base + far * CHUNKS + h, (core, f))

    def ag_wait(ref, base, b):
        for h in range(CHUNKS):
            arrive(ref.at[b, h * step : (h + 1) * step], base + b * CHUNKS + h)

    def rs_send(P, L1, L2, base, compute):
        for j, hi in enumerate((1 - x, x)):
            b_send, b_keep = hi * 2 + 1 - c, hi * 2 + c
            compute(b_send)
            push(P.at[b_send], L1.at[j], base + j, (core, f))
            if j == 0:
                compute(b_keep)
        b_far = (1 - x) * 2 + c
        arrive(L1.at[0], base)
        P[b_far] = (P[b_far].astype(f32) + L1[0].astype(f32)).astype(bf16)
        push(P.at[b_far], L2, base + 2, (far, f))
        compute(d)

    def rs_total(P, L1, L2, base):
        arrive(L1.at[1], base + 1)
        arrive(L2, base + 2)
        return P[d].astype(f32) + L1[1].astype(f32) + L2[...].astype(f32)

    def lines(b):
        return pl.ds(pl.multiple_of(b * own, own), own)

    def tile(i):
        return slice(i * part, (i + 1) * part)

    ag1, agc, ag2, agp = slots(dpn * CHUNKS), slots(dpn * CHUNKS), slots(dpn * CHUNKS), slots(dpn * CHUNKS)
    rs1, rs2, rs3, rs4 = slots(3), slots(3), slots(3), slots(3)

    N1[d] = (N1F[...] * VEC[0:1, :] + VEC[1:2, :]).astype(bf16)
    COT[d] = cot[...]
    ag_start(N1, ag1)
    forward(q_at, zq, yq)
    forward(o_at, zo, yo, 1, 1)
    across_own(u_at, yu)
    ag_forward(N1, ag1)
    ag_start(COT, agc)
    forward(o_at, zo, yo, 2)
    gathered(q_at, yq)
    for n, b in enumerate(order):
        if n in (1, 3):
            ag_wait(N1, ag1, b)
        QKV[lines(b), :] = dot(N1[b], WQ[...].reshape(width, 3 * part), 1, 0).astype(bf16)
    forward(u_at, zu, yu, 1, 1)
    attn_fwd_kernel(lens, QKV, ATT, LSE, {1: lambda: forward(u_at, zu, yu, 2, 2)})
    ag_forward(COT, agc)
    gathered(o_at, yo)

    def proj(b):
        PA[b] = dot(ATT[lines(b), :], WO[...].reshape(part, width), 1, 0).astype(bf16)

    proj_sends = len(sent)
    rs_send(PA, LA1, LA2, rs1, proj)
    proj_sends = sent[proj_sends:]
    forward(u_at, zu, yu, 3)
    MID[...] = frames[...].astype(f32) + rs_total(PA, LA1, LA2, rs1)
    norm_rows(MID[...], N2F, INV2)
    NORM2[d] = (N2F[...] * VEC[2:3, :] + VEC[3:4, :]).astype(bf16)
    ag_start(NORM2, ag2)
    forward(d_at, zd, yd, 1, 1)
    gathered(u_at, yu)

    def up(b):
        for i in range(dpn):
            u = dot(NORM2[b], WU[:, :, :, tile(i)].reshape(width, part), 1, 0)
            cdf = 0.5 * (1.0 + lax.erf(u * (0.5**0.5)))
            ACT[b, :, tile(i)] = (u * cdf).astype(bf16)
            SLOPE[b, :, tile(i)] = cdf + u * (jnp.exp(-0.5 * u * u) * (1.0 / (2.0 * jnp.pi) ** 0.5))

    up(d)
    ag_wait(NORM2, ag2, core)
    up(core)
    ag_forward(NORM2, ag2)
    up(far)
    forward(d_at, zd, yd, 2, 2)
    ag_wait(NORM2, ag2, other)
    up(other)
    forward(d_at, zd, yd, 3)
    ag_wait(COT, agc, core)
    ag_wait(COT, agc, other)
    y_d, y_u, y_o, y_q = slots(nz), slots(dpn), slots(1), slots(dpn)
    z_d, z_u, z_o, z_q = slots(nz), slots(nz * dpn), slots(nz), slots(nz * dpn)
    big = wd_in.shape[0]

    def against(a, b, i):
        return dot(a[:, :, tile(i)].reshape(dpn * own, part), b, 0, 0).astype(bf16)

    for k in range(1, nz + 1):
        j = zpeer(k)
        a = ACT[:, :, pl.ds(pl.multiple_of(j * part, part), part)].reshape(dpn * own, part)
        GD[j] = dot(a, COT[...].reshape(dpn * own, width), 0, 0).astype(bf16).reshape(2, big, width)
        push(GD.at[j, 1 - y], YD.at[j], y_d + j, pair)
    gathered(d_at, yd)
    per = fsn // dpn

    def grad_hidden(b):
        for i in range(dpn):
            g = dot(COT[b], WD[i * per : (i + 1) * per].reshape(part, width), 1, 1)
            GUP[b, :, tile(i)] = (g * SLOPE[b, :, tile(i)]).astype(bf16)
        for i in range(dpn):
            PB[b, :, tile(i)] = dot(GUP[b], WU[i].reshape(part, width), 1, 1).astype(bf16)

    norm2_sends = len(sent)
    rs_send(PB, LB1, LB2, rs2, grad_hidden)
    norm2_sends = sent[norm2_sends:]

    def add(a, b):
        return (a.astype(f32) + b.astype(f32)).astype(bf16)

    def sum_d(k):
        j = zpeer(k)
        arrive(YD.at[j], y_d + j)
        YD[j] = add(GD[j, y], YD[j])
        if k < nz:
            push(YD.at[j], ZD.at[z], z_d + z, (d, j * 2 + y))

    def sum_chunk(G, Y, S, Z, ys, zs, i):
        arrive(Y.at[i], ys + i)
        S[:, i] = add(G[i, :, y], Y[i])
        for k in range(1, nz):
            zz = zpeer(k)
            push(S.at[zz, i], Z.at[z, i], zs + z * dpn + i, (d, zz * 2 + y))

    def sum_u(i):
        sum_chunk(GU, YU, SU, ZU, y_u, z_u, i)

    def sum_q(i):
        sum_chunk(GQ, YQ, SQ, ZQ, y_q, z_q, i)

    sum_d(1)
    MIDG = N2F
    grad2 = rs_total(PB, LB1, LB2, rs2)
    mid_norm, gain2, bias2 = norm_back(N2F[...], INV2[...], VEC[2:3, :], grad2)
    MIDG[...] = cot[...].astype(f32) + mid_norm
    GPROJ[d] = MIDG[...].astype(bf16)
    ag_start(GPROJ, agp)

    sent_out(proj_sends)

    for i in range(dpn):
        g = against(NORM2, GUP[...].reshape(dpn * own, width), i)
        GU[i] = g.reshape(nz, 2, rows, width)
        push(GU.at[i, :, 1 - y], YU.at[i], y_u + i, pair)

    def grad_heads(b):
        GATT[lines(b), :] = dot(GPROJ[b], WO[...].reshape(part, width), 1, 1).astype(bf16)

    sum_d(2)
    grad_heads(d)
    ag_forward(GPROJ, agp)
    sum_d(3)
    grad_heads(far)
    ag_wait(GPROJ, agp, core)
    grad_heads(core)
    ag_wait(GPROJ, agp, other)
    grad_heads(other)

    g = dot(ATT[...], GPROJ[...].reshape(dpn * own, width), 0, 0).astype(bf16)
    GO[...] = g.reshape(nz, 2, rows, width)
    push(GO.at[:, 1 - y], YO, y_o, pair)
    sum_d(nz)

    attn_bwd_kernel(lens, QKV, GATT, LSE, GQKV, DK, DV, {1: lambda: sum_u(0)})

    for i in range(dpn):
        g = against(N1, GQKV[...], i)
        GQ[i] = g.reshape(nz, 2, rows, 3 * part)
        push(GQ.at[i, :, 1 - y], YQ.at[i], y_q + i, pair)
    for i in range(1, dpn):
        sum_u(i)

    sent_out(norm2_sends)

    def grad_first(b):
        for i in range(dpn):
            PB[b, :, tile(i)] = dot(GQKV[lines(b), :], WQ[i].reshape(part, 3 * part), 1, 1).astype(bf16)

    rs_send(PB, LD1, LD2, rs4, grad_first)

    def down(b):
        PA[b] = dot(ACT[b], WD[...].reshape(width, width), 1, 0).astype(bf16)

    rs_send(PA, LC1, LC2, rs3, down)

    arrive(YO, y_o)
    YO[...] = add(GO[:, y], YO[...])
    for k in range(1, nz):
        zz = zpeer(k)
        push(YO.at[zz], ZO.at[z], z_o + z, (d, zz * 2 + y))
    for i in range(dpn):
        sum_q(i)
    SD, SO = YD, YO

    def settle(S, Z, zs, pieces=1):
        total = S[z].astype(f32)
        for k in range(1, nz):
            zz = zpeer(k)
            for i in range(pieces):
                arrive(Z.at[zz, i] if pieces > 1 else Z.at[zz], zs + zz * pieces + i)
            total = total + Z[zz].astype(f32)
        return total

    back_u, back_q = slots(dpn), slots(dpn)
    TU[...] = settle(SU, ZU, z_u, dpn).astype(bf16)
    for k in range(1, dpn):
        dd = lax.rem(d + k, dpn)
        push(TU.at[dd], RU.at[d], back_u + d, (dd, f))
    RU[d] = TU[d]

    grad1 = rs_total(PB, LD1, LD2, rs4)
    in_norm, gain1, bias1 = norm_back(N1F[...], INV1[...], VEC[0:1, :], grad1)
    o_in[...] = MIDG[...] + in_norm
    small = jnp.concatenate([v.reshape(1, width) for v in (gain1, bias1, gain2, bias2)] + [jnp.zeros((4, width), f32)], axis=0)
    for i in range(dpn):
        SM[i] = small[:, tile(i)]
    sm_d, sm_y, sm_z = slots(dpn), slots(1), slots(nz)
    for k in range(1, dpn):
        dd = lax.rem(d + k, dpn)
        push(SM.at[dd], SM1.at[d], sm_d + d, (dd, f))

    o_d[...] = settle(SD, ZD, z_d)
    o_o[...] = settle(SO, ZO, z_o)

    total = SM[d]
    for k in range(1, dpn):
        s = lax.rem(d + k, dpn)
        arrive(SM1.at[s], sm_d + s)
        total = total + SM1[s]
    SM2[...] = total
    push(SM2, SM3, sm_y, pair)

    arrive(SM3, sm_y)
    SM4[...] = SM2[...] + SM3[...]
    for k in range(1, nz):
        push(SM4, SM5.at[z], sm_z + z, (d, zpeer(k) * 2 + y))

    TQ[...] = settle(SQ, ZQ, z_q, dpn).astype(bf16)
    for k in range(1, dpn):
        dd = lax.rem(d + k, dpn)
        push(TQ.at[dd], RQ.at[d], back_q + d, (dd, f))
    RQ[d] = TQ[d]

    o_res[...] = (MID[...] + rs_total(PA, LC1, LC2, rs3)).astype(bf16)
    for k in range(1, dpn):
        s = lax.rem(d + k, dpn)
        arrive(RU.at[s], back_u + s)
    for s in range(dpn):
        o_u[:, s * width : (s + 1) * width] = RU[s].astype(f32)
    for k in range(1, dpn):
        s = lax.rem(d + k, dpn)
        arrive(RQ.at[s], back_q + s)
    for s in range(dpn):
        for j in range(3):
            o_q[:, j * width + s * part : j * width + (s + 1) * part] = RQ[s, :, tile(j)].astype(f32)
    total = SM4[...]
    for k in range(1, nz):
        zz = zpeer(k)
        arrive(SM5.at[zz], sm_z + zz)
        total = total + SM5[zz]
    o_small[...] = total

    waited = set(id(copy) for _, copy in proj_sends + norm2_sends)
    sent_out([(when, copy) for when, copy in sent if id(copy) not in waited])


def in_one_kernel(frames, cotangent, phon_len, acou_len, row_item, w_qkv, w_out, w_up, w_down, ln1_gain, ln1_bias, ln2_gain, ln2_bias):
    dpn, fsn = lax.axis_size("dp"), lax.axis_size("fsdp")
    nz = fsn // 2
    own, width = frames.shape[1:]
    length = dpn * own
    part = width // dpn
    rows = w_up.shape[0]
    big = w_down.shape[0]
    item = row_item[0]
    pick = jnp.arange(phon_len.shape[0], dtype=jnp.int32) == item
    lens = jnp.stack([jnp.sum(jnp.where(pick, phon_len, 0)), jnp.sum(jnp.where(pick, acou_len, 0))])
    place = lax.axis_index("fsdp") * rows % 128
    vec = jnp.stack([ln1_gain, ln1_bias, ln2_gain, ln2_bias]).astype(f32)
    vec = jnp.pad(vec, ((0, 4), (0, 128 - rows)))
    vec = jnp.roll(vec, place, axis=1)
    wq = w_qkv.reshape(rows, 3, dpn, part).transpose(2, 0, 1, 3).reshape(dpn, rows, 3 * part)
    wu = w_up.reshape(rows, dpn, width).transpose(1, 0, 2)

    def buf(*shape, dtype=bf16):
        return pltpu.VMEM(shape, dtype)

    full = buf(dpn, own, width)
    land = [buf(2, own, width), buf(own, width)]
    scratch = [
        buf(dpn, fsn, 8, 128, dtype=f32), buf(8, width, dtype=f32),
        buf(dpn, fsn, rows, 3 * part), buf(fsn, rows, width), buf(dpn, fsn, rows, width), buf(fsn, big, width),
        buf(own, width, dtype=f32), buf(own, 1, dtype=f32), full, full,
        buf(length, 3 * part), buf(length, part), buf(8, length, dtype=f32), full, full,
        *land, *land, *land, *land,
        buf(own, width, dtype=f32), buf(own, width, dtype=f32), buf(own, 1, dtype=f32),
        full, full, buf(dpn, own, width, dtype=f32), full, full,
        buf(length, part), buf(length, 3 * part), buf(length, part, dtype=f32), buf(length, part, dtype=f32),
        buf(nz, 2, big, width), buf(dpn, nz, 2, rows, width), buf(nz, 2, rows, width), buf(dpn, nz, 2, rows, 3 * part),
        buf(nz, big, width), buf(dpn, nz, rows, width), buf(nz, rows, width), buf(dpn, nz, rows, 3 * part),
        buf(nz, dpn, rows, width), buf(nz, dpn, rows, 3 * part),
        buf(nz, big, width), buf(nz, dpn, rows, width), buf(nz, rows, width), buf(nz, dpn, rows, 3 * part),
        buf(dpn, rows, width), buf(dpn, rows, 3 * part), buf(dpn, rows, width), buf(dpn, rows, 3 * part),
        buf(dpn, 8, part, dtype=f32), buf(dpn, 8, part, dtype=f32), buf(8, part, dtype=f32), buf(8, part, dtype=f32),
        buf(8, part, dtype=f32), buf(nz, 8, part, dtype=f32),
        pltpu.SemaphoreType.DMA((SENDS,)), pltpu.SemaphoreType.DMA((ARRIVALS,)),
    ]
    outs = pl.pallas_call(
        layer_kernel,
        out_shape=(
            jax.ShapeDtypeStruct((own, width), bf16),
            jax.ShapeDtypeStruct((own, width), f32),
            jax.ShapeDtypeStruct((rows, 3 * width), f32),
            jax.ShapeDtypeStruct((rows, width), f32),
            jax.ShapeDtypeStruct((rows, dpn * width), f32),
            jax.ShapeDtypeStruct((big, width), f32),
            jax.ShapeDtypeStruct((8, part), f32),
        ),
        in_specs=[SMEM] + [VMEM] * 7,
        out_specs=(VMEM,) * 7,
        scratch_shapes=scratch,
        compiler_params=pltpu.CompilerParams(collective_id=0, has_side_effects=True, vmem_limit_bytes=67043328),
        name="layer",
    )(lens, frames[0], cotangent[0], vec, wq, w_out, wu, w_down)
    small = lax.dynamic_slice(outs[6], (0, lax.axis_index("fsdp") * rows), (4, rows))
    return (outs[0][None], outs[1][None], *outs[2:6], small[0], small[1], small[2], small[3])


def on_device(*args):
    dpn, fsn, rows, width = lax.axis_size("dp"), lax.axis_size("fsdp"), args[7].shape[0], args[0].shape[2]
    fits = dpn == 4 and fsn % dpn == 0 and rows % 16 == 0 and 128 % rows == 0 and width == 2 * dpn * args[8].shape[0]
    return (in_one_kernel if fits else with_collectives)(*args)


def solution(mesh):
    split = P(("dp", "fsdp"), None)
    vec = P(("dp", "fsdp"))
    acts = P("fsdp", "dp", None)
    return jax.shard_map(
        on_device,
        mesh=mesh,
        in_specs=(acts, acts, P(), P(), P("fsdp"), split, split, split, split, vec, vec, vec, vec),
        out_specs=(acts, acts, split, split, split, split, vec, vec, vec, vec),
        check_vma=False,
    )
```

```python
import functools

import jax
import jax.numpy as jnp
from jax import lax
from jax.experimental import pallas as pl
from jax.experimental.pallas import tpu as pltpu
from jax.sharding import PartitionSpec as P

HEAD_DIM = 64
EPS = 1e-05
MASKED = -1e30
BLOCK = 256

f32 = jnp.float32
bf16 = jnp.bfloat16


def dot(a, b, ca, cb):
    return lax.dot_general(a, b, (((ca,), (cb,)), ((), ())), preferred_element_type=f32)


def row_limit(start, rows, phon, acou):
    pos = start + lax.broadcasted_iota(jnp.int32, (1, rows), 1)
    return jnp.where(pos < phon + acou, jnp.maximum(pos, phon - 1), phon - 1)


def head_mask(width, head):
    lane = lax.broadcasted_iota(jnp.int32, (1, width), 1)
    return (lane >= head * HEAD_DIM) & (lane < (head + 1) * HEAD_DIM)


def attn_fwd_kernel(lens, qkv, out, lse, between={}):
    width = out.shape[1]
    heads = width // HEAD_DIM
    length = out.shape[0]
    phon, acou = lens[0], lens[1]
    scale = HEAD_DIM ** (-0.5)
    for start in range(0, length, BLOCK):
        if start // BLOCK in between:
            between[start // BLOCK]()
        seen = start + BLOCK
        q = qkv[start : start + BLOCK, :width] * scale
        k = qkv[:seen, width : 2 * width]
        v = qkv[:seen, 2 * width :]
        limit = row_limit(start, BLOCK, phon, acou)
        key = lax.broadcasted_iota(jnp.int32, (seen, 1), 0)
        hidden = key > limit
        total = jnp.zeros((BLOCK, width), f32)
        rows = []
        for h in range(heads):
            mine = head_mask(width, h)
            qh = jnp.where(mine, q, 0)
            s = dot(k, qh, 1, 1)
            s = jnp.where(hidden, MASKED, s)
            top = jnp.max(s, axis=0, keepdims=True)
            e = jnp.exp(s - top)
            tot = jnp.sum(e, axis=0, keepdims=True)
            p = (e * (1.0 / tot)).astype(bf16)
            o = dot(p, v, 0, 0)
            total = total + jnp.where(mine, o, 0)
            rows.append(top + jnp.log(tot))
        out[start : start + BLOCK, :] = total.astype(bf16)
        lse[:, start : start + BLOCK] = jnp.concatenate(rows + [jnp.zeros((8 - heads, BLOCK), f32)], axis=0)


def attn_bwd_kernel(lens, qkv, grad, lse, dqkv, dk_acc, dv_acc, between={}):
    width = grad.shape[2]
    heads = width // HEAD_DIM
    length = grad.shape[0] * BLOCK
    phon, acou = lens[0], lens[1]
    scale = HEAD_DIM ** (-0.5)
    dk_acc[...] = jnp.zeros_like(dk_acc)
    dv_acc[...] = jnp.zeros_like(dv_acc)
    for start in reversed(range(0, length, BLOCK)):
        if start // BLOCK in between:
            between[start // BLOCK]()
        seen = start + BLOCK
        limit = row_limit(start, BLOCK, phon, acou)

        def two_heads(two, dq):
            q = qkv[start : start + BLOCK, :width] * scale
            g = grad[start // BLOCK]
            k = qkv[:seen, width : 2 * width]
            v = qkv[:seen, 2 * width :]
            hidden = lax.broadcasted_iota(jnp.int32, (seen, 1), 0) > limit
            for h in (2 * two, 2 * two + 1):
                mine = head_mask(width, h)
                qh = jnp.where(mine, q, 0)
                gh = jnp.where(mine, g, 0)
                s = dot(k, qh, 1, 1)
                s = jnp.where(hidden, MASKED, s)
                p = jnp.exp(s - lse[pl.ds(h, 1), start : start + BLOCK])
                gp = dot(v, gh, 1, 1)
                delta = jnp.sum(p * gp, axis=0, keepdims=True)
                ds = (p * (gp - delta)).astype(bf16)
                dvh = dot(p.astype(bf16), gh, 1, 0)
                dkh = dot(ds, qh, 1, 0)
                dv_acc[: seen // BLOCK] += dvh.reshape(seen // BLOCK, BLOCK, width)
                dk_acc[: seen // BLOCK] += dkh.reshape(seen // BLOCK, BLOCK, width)
                dq = dq + jnp.where(mine, dot(ds, k, 0, 0), 0)
            return dq

        dq = lax.fori_loop(0, heads // 2, two_heads, jnp.zeros((BLOCK, width), f32))
        dqkv[start // BLOCK, :, :width] = (dq * scale).astype(bf16)
    dqkv[:, :, width : 2 * width] = dk_acc[...].astype(bf16)
    dqkv[:, :, 2 * width :] = dv_acc[...].astype(bf16)


VMEM = pl.BlockSpec(memory_space=pltpu.VMEM)
SMEM = pl.BlockSpec(memory_space=pltpu.SMEM)


def attn_fwd(lens, qkv):
    length, width = qkv.shape[0], qkv.shape[1] // 3
    return pl.pallas_call(
        attn_fwd_kernel,
        out_shape=(jax.ShapeDtypeStruct((length, width), bf16), jax.ShapeDtypeStruct((8, length), f32)),
        in_specs=[SMEM, VMEM],
        out_specs=(VMEM, VMEM),
        compiler_params=pltpu.CompilerParams(vmem_limit_bytes=40 * 2**20),
        cost_estimate=pl.CostEstimate(flops=4 * length * length * width, bytes_accessed=8 * length * width, transcendentals=length * length * width // HEAD_DIM),
        name="attn_fwd",
    )(lens, qkv)


def attn_bwd(lens, qkv, grad, lse):
    length, width = grad.shape
    blocks = length // BLOCK
    out = pl.pallas_call(
        attn_bwd_kernel,
        out_shape=jax.ShapeDtypeStruct((blocks, BLOCK, 3 * width), bf16),
        in_specs=[SMEM, VMEM, VMEM, VMEM],
        out_specs=VMEM,
        scratch_shapes=[pltpu.VMEM((blocks, BLOCK, width), f32)] * 2,
        compiler_params=pltpu.CompilerParams(vmem_limit_bytes=40 * 2**20),
        cost_estimate=pl.CostEstimate(flops=10 * length * length * width, bytes_accessed=14 * length * width, transcendentals=length * length * width // HEAD_DIM),
        name="attn_bwd",
    )(lens, qkv, grad.reshape(blocks, BLOCK, width), lse)
    return out.reshape(length, 3 * width)


def norm_parts(v):
    mean = jnp.mean(v, axis=-1, keepdims=True)
    centered = v - mean
    var = jnp.mean(centered * centered, axis=-1, keepdims=True)
    inv = lax.rsqrt(var + EPS)
    return centered * inv, inv


def norm_back(n, inv, gain, grad):
    g = grad * gain
    dx = inv * (g - jnp.mean(g, axis=-1, keepdims=True) - n * jnp.mean(g * n, axis=-1, keepdims=True))
    return dx, jnp.sum(grad * n, axis=0), jnp.sum(grad, axis=0)


def with_collectives(frames, cotangent, phon_len, acou_len, row_item, w_qkv, w_out, w_up, w_down, ln1_gain, ln1_bias, ln2_gain, ln2_bias):
    tp, dpn, fsn = "dp", lax.axis_size("dp"), lax.axis_size("fsdp")
    width = frames.shape[2]
    part = width // dpn
    rows = w_up.shape[0]

    vecs = jnp.concatenate([ln1_gain, ln1_bias, ln2_gain, ln2_bias])[None]
    vecs = lax.all_gather(vecs, ("dp", "fsdp"), axis=0, tiled=True)
    vecs = vecs.reshape(dpn * fsn, 4, rows).transpose(1, 0, 2).reshape(4, width).astype(f32)

    qkv_cols = w_qkv.reshape(rows, 3, dpn, part).transpose(2, 0, 1, 3).reshape(dpn, rows, 3 * part)
    qkv_cols = lax.all_to_all(qkv_cols, tp, 0, 0, tiled=True)
    wq = lax.all_gather(qkv_cols, "fsdp", axis=1, tiled=True).reshape(width, 3 * part)
    wo = lax.all_gather(w_out, "fsdp", axis=0, tiled=True)
    ff = w_up.shape[1] // dpn
    up_cols = w_up.reshape(rows, dpn, ff).transpose(1, 0, 2)
    up_cols = lax.all_to_all(up_cols, tp, 0, 0, tiled=True)
    wu = lax.all_gather(up_cols, "fsdp", axis=1, tiled=True).reshape(width, ff)
    wd = lax.all_gather(w_down, "fsdp", axis=0, tiled=True)

    item = row_item[0]
    pick = jnp.arange(phon_len.shape[0], dtype=jnp.int32) == item
    lens = jnp.stack([jnp.sum(jnp.where(pick, phon_len, 0)), jnp.sum(jnp.where(pick, acou_len, 0))])

    x = frames[0].astype(f32)
    n1, inv1 = norm_parts(x)
    normed1 = lax.all_gather((n1 * vecs[0] + vecs[1]).astype(bf16), tp, axis=0, tiled=True)
    grad_down = lax.all_gather(cotangent[0], tp, axis=0, tiled=True)
    qkv = jnp.dot(normed1, wq, preferred_element_type=f32).astype(bf16)
    attn_out, lse = attn_fwd(lens, qkv)
    proj = jnp.dot(attn_out, wo, preferred_element_type=f32).astype(bf16)
    middle = x + lax.psum_scatter(proj, tp, scatter_dimension=0, tiled=True).astype(f32)
    n2, inv2 = norm_parts(middle)
    normed2 = lax.all_gather((n2 * vecs[2] + vecs[3]).astype(bf16), tp, axis=0, tiled=True)
    up_out = jnp.dot(normed2, wu, preferred_element_type=f32)
    cdf = 0.5 * (1.0 + lax.erf(up_out * (0.5**0.5)))
    act_out = (up_out * cdf).astype(bf16)
    down = jnp.dot(act_out, wd, preferred_element_type=f32).astype(bf16)
    result = (middle + lax.psum_scatter(down, tp, scatter_dimension=0, tiled=True).astype(f32)).astype(bf16)

    g_down = dot(act_out, grad_down, 0, 0).astype(bf16)
    slope = cdf + up_out * (jnp.exp(-0.5 * up_out * up_out) * (1.0 / (2.0 * jnp.pi) ** 0.5))
    grad_up = (dot(grad_down, wd, 1, 1) * slope).astype(bf16)
    g_up = dot(normed2, grad_up, 0, 0).astype(bf16)
    grad_norm2 = lax.psum_scatter(dot(grad_up, wu, 1, 1).astype(bf16), tp, scatter_dimension=0, tiled=True).astype(f32)
    mid_norm, g_gain2, g_bias2 = norm_back(n2, inv2, vecs[2], grad_norm2)
    grad_middle = cotangent[0].astype(f32) + mid_norm
    grad_proj = lax.all_gather(grad_middle.astype(bf16), tp, axis=0, tiled=True)
    g_out = dot(attn_out, grad_proj, 0, 0).astype(bf16)
    grad_attn = dot(grad_proj, wo, 1, 1).astype(bf16)
    grad_qkv = attn_bwd(lens, qkv, grad_attn, lse)
    g_qkv = dot(normed1, grad_qkv, 0, 0).astype(bf16)
    grad_norm1 = lax.psum_scatter(dot(grad_qkv, wq, 1, 1).astype(bf16), tp, scatter_dimension=0, tiled=True).astype(f32)
    in_norm, g_gain1, g_bias1 = norm_back(n1, inv1, vecs[0], grad_norm1)
    grad_inputs = grad_middle + in_norm

    def owned_rows(g):
        return lax.psum_scatter(g, "fsdp", scatter_dimension=0, tiled=True)

    def owned_cols(g, groups):
        g = lax.psum_scatter(g.reshape(dpn, width // dpn, -1), "fsdp", scatter_dimension=1, tiled=True)
        g = lax.all_to_all(g, tp, 0, 0, tiled=True)
        g = g.reshape(dpn, rows, groups, -1).transpose(1, 2, 0, 3)
        return g.reshape(rows, -1).astype(f32)

    o_down = owned_rows(g_down).astype(f32)
    o_up = owned_cols(g_up, 1)
    o_out = owned_rows(g_out).astype(f32)
    o_qkv = owned_cols(g_qkv, 3)
    small = jnp.stack([g_gain1, g_bias1, g_gain2, g_bias2]).reshape(4, dpn * fsn, rows).transpose(1, 0, 2)
    small = lax.psum_scatter(small.reshape(dpn * fsn, 4 * rows), ("dp", "fsdp"), scatter_dimension=0, tiled=True).reshape(4, rows)
    return (result[None], grad_inputs[None], o_qkv, o_out, o_up, o_down, small[0], small[1], small[2], small[3])


CHUNKS = 2
SENDS = 320
ARRIVALS = 320
MESH = pl.DeviceIdType.MESH


def layer_kernel(
    phon_len, acou_len, row_item, frames, cot, vec_in, wq_in, wo_in, wu_in, wd_in,
    o_res, o_in, o_q, o_o, o_u, o_d, o_small,
    VG, VEC, WQ, WO, WU, WD, N1F, INV1, N1, COT, QKV, ATT, LSE, PA, PB,
    LA1, LA2, LB1, LB2, LC1, LC2, LD1, LD2,
    MID, N2F, INV2, NORM2, ACT, SLOPE, GUP, GPROJ,
    GD, GU, GO, GQ, YD, YU, YO, YQ, SU, SQ, ZD, ZU, ZO, ZQ, RU, RQ,
    SM, SM1, SM2, SM3, SM4, SM5,
    ssem, rsem,
):
    dpn, fsn = lax.axis_size("dp"), lax.axis_size("fsdp")
    lens = (phon_len[row_item[0]], acou_len[row_item[0]])
    nz = fsn // 2
    width = frames.shape[1]
    own = frames.shape[0]
    part = width // dpn
    rows = wu_in.shape[0]
    d, f = lax.axis_index("dp"), lax.axis_index("fsdp")
    c, x = lax.rem(d, 2), lax.div(d, 2)
    y, z = lax.rem(f, 2), lax.div(f, 2)
    core = d + 1 - 2 * c
    far = lax.rem(d + 2, dpn)
    other = lax.rem(core + 2, dpn)
    order = (d, core, far, other)
    pair = (d, f + 1 - 2 * y)
    count = {"send": 0, "arrive": 0}
    sent = []

    def slots(n):
        base = count["arrive"]
        count["arrive"] += n
        assert count["arrive"] <= ARRIVALS
        return base

    def push(src, dst, slot, device, when=None):
        i = count["send"]
        count["send"] += 1
        assert i < SENDS
        copy = pltpu.make_async_remote_copy(src, dst, ssem.at[i], rsem.at[slot], device_id=device, device_id_type=MESH)
        if when is None:
            copy.start()
        else:
            pl.when(when)(lambda: copy.start())
        sent.append((when, copy))

    def push_each(n, piece, compute):
        first = count["send"]
        count["send"] += n

        def copy_of(i):
            src, dst, slot, device = piece(i)
            return pltpu.make_async_remote_copy(src, dst, ssem.at[first + i], rsem.at[slot], device_id=device, device_id_type=MESH)

        def step(i, carry):
            compute(i)
            copy_of(i).start()
            return carry

        lax.fori_loop(0, n, step, 0)
        sent.extend((None, copy_of(i)) for i in range(n))

    def sent_out(copies):
        for when, copy in copies:
            if when is None:
                copy.wait_send()
            else:
                pl.when(when)(lambda copy=copy: copy.wait_send())

    def arrive(ref, slot):
        pltpu.make_async_remote_copy(ref, ref, ssem.at[0], rsem.at[slot], device_id=pair, device_id_type=MESH).wait_recv()

    def zpeer(k):
        return lax.rem(z + k, nz)

    barrier = pltpu.get_barrier_semaphore()
    peers = [(lax.rem(d + k, dpn), f) for k in range(1, dpn)] + [(d, lax.rem(f + k, fsn)) for k in range(1, fsn)]
    for device in peers:
        pl.semaphore_signal(barrier, inc=1, device_id=device, device_id_type=MESH)
    pl.semaphore_wait(barrier, len(peers))

    def tile(i):
        return slice(i * part, (i + 1) * part)

    vec_f, vec_d = slots(fsn), slots(dpn)
    for k in range(1, fsn):
        push(vec_in, VG.at[d, f], vec_f + f, (d, lax.rem(f + k, fsn)))
    mix_q, mix_u = slots(dpn * 3), slots(dpn)

    def q_cols(dd, j):
        return pl.ds(pl.multiple_of(j * width + dd * part, part), part)

    def u_cols(dd):
        return pl.ds(pl.multiple_of(dd * width, width), width)

    for k in range(1, dpn):
        dd = lax.rem(d + k, dpn)
        for j in range(3):
            push(wq_in.at[:, q_cols(dd, j)], WQ.at[d, f, :, tile(j)], mix_q + d * 3 + j, (dd, f))
    for k in range(1, dpn):
        dd = lax.rem(d + k, dpn)
        push(wu_in.at[:, u_cols(dd)], WU.at[d, f], mix_u + d, (dd, f))
    zq, zo, zu, zd = slots(nz), slots(nz), slots(nz), slots(nz)
    yq, yo, yu, yd = slots(nz), slots(nz), slots(nz), slots(nz)
    def clip(v):
        return jnp.clip(v, 0, nz - 1)

    def along(ref_at, zs):
        for side in (1, -1):
            to = z + side
            push(ref_at(f), ref_at(f), zs + z, (d, clip(to) * 2 + y), when=(to >= 0) & (to < nz))

    def across_own(ref_at, ys):
        push(ref_at(f), ref_at(f), ys + z, pair)

    def hop(ref_at, zs, ys, h):
        for side in (1, -1):
            src, to = z + side * h, z - side
            here = (src >= 0) & (src < nz)
            ref, src = ref_at(clip(src) * 2 + y), clip(src)
            pl.when(here)(lambda: arrive(ref, zs + src))
            push(ref, ref, zs + src, (d, clip(to) * 2 + y), when=here & (to >= 0) & (to < nz))
            push(ref, ref, ys + src, pair, when=here)

    def forward(ref_at, zs, ys, first=1, last=None):
        for h in range(first, nz if last is None else last + 1):
            hop(ref_at, zs, ys, h)

    def gathered(ref_at, ys):
        for zz in range(nz):
            arrive(ref_at(2 * zz + 1 - y), ys + zz)

    def q_at(s):
        return WQ.at[:, s]

    def o_at(s):
        return WO.at[s]

    def u_at(s):
        return WU.at[:, s]

    def d_at(s):
        return WD.at[s]

    WO[f] = wo_in[...]
    WD[f] = wd_in[...]
    along(o_at, zo)
    across_own(o_at, yo)
    across_own(d_at, yd)
    VG[d, f] = vec_in[...]
    for j in range(3):
        WQ[d, f, :, tile(j)] = wq_in[:, q_cols(d, j)]
    WU[d, f] = wu_in[:, u_cols(d)]

    def norm_rows(v, nf, inv):
        n, i = norm_parts(v)
        nf[...] = n
        inv[...] = i

    norm_rows(frames[...].astype(f32), N1F, INV1)
    for k in range(1, fsn):
        s = lax.rem(f + k, fsn)
        arrive(VG.at[d, s], vec_f + s)
    for k in range(1, dpn):
        push(VG.at[d], VG.at[d], vec_d + d, (lax.rem(d + k, dpn), f))

    for k in range(1, dpn):
        s = lax.rem(d + k, dpn)
        for j in range(3):
            arrive(WQ.at[s, f, :, tile(j)], mix_q + s * 3 + j)
    along(q_at, zq)
    across_own(q_at, yq)
    for k in range(1, dpn):
        s = lax.rem(d + k, dpn)
        arrive(VG.at[s], vec_d + s)
    group = 128 // rows
    for m in range(width // 128):
        total = VG[(m * group) // fsn, (m * group) % fsn]
        for j in range(1, group):
            total = total + VG[(m * group + j) // fsn, (m * group + j) % fsn]
        VEC[:, m * 128 : (m + 1) * 128] = total

    step = own // CHUNKS

    def ag_start(ref, base):
        for device in (far, core):
            for h in range(CHUNKS):
                piece = ref.at[d, h * step : (h + 1) * step]
                push(piece, piece, base + d * CHUNKS + h, (device, f))

    def ag_forward(ref, base):
        for h in range(CHUNKS):
            piece = ref.at[far, h * step : (h + 1) * step]
            arrive(piece, base + far * CHUNKS + h)
            push(piece, piece, base + far * CHUNKS + h, (core, f))

    def ag_wait(ref, base, b):
        for h in range(CHUNKS):
            arrive(ref.at[b, h * step : (h + 1) * step], base + b * CHUNKS + h)

    def rs_near(P, L1, base, compute, between=lambda: None):
        for j, hi in enumerate((1 - x, x)):
            b_send, b_keep = hi * 2 + 1 - c, hi * 2 + c
            compute(b_send)
            push(P.at[b_send], L1.at[j], base + j, (core, f))
            compute(b_keep)
            if j == 0:
                between()

    def rs_far(P, L1, L2, base):
        b_far = (1 - x) * 2 + c
        arrive(L1.at[0], base)
        P[b_far] = (P[b_far].astype(f32) + L1[0].astype(f32)).astype(bf16)
        push(P.at[b_far], L2, base + 2, (far, f))

    def rs_send(P, L1, L2, base, compute):
        rs_near(P, L1, base, compute, lambda: rs_far(P, L1, L2, base))

    def rs_total(P, L1, L2, base):
        arrive(L1.at[1], base + 1)
        arrive(L2, base + 2)
        return P[d].astype(f32) + L1[1].astype(f32) + L2[...].astype(f32)

    def lines(b):
        return pl.ds(pl.multiple_of(b * own, own), own)

    ag1, agc, ag2, agp = slots(dpn * CHUNKS), slots(dpn * CHUNKS), slots(dpn * CHUNKS), slots(dpn * CHUNKS)
    rs1, rs2, rs3, rs4 = slots(3), slots(3), slots(3), slots(3)

    N1[d] = (N1F[...] * VEC[0:1, :] + VEC[1:2, :]).astype(bf16)
    COT[d] = cot[...]
    ag_start(N1, ag1)
    forward(q_at, zq, yq, 1, 1)
    forward(o_at, zo, yo, 1, 1)
    forward(q_at, zq, yq, 2, 2)
    forward(o_at, zo, yo, 2, 2)
    for k in range(1, dpn):
        s = lax.rem(d + k, dpn)
        arrive(WU.at[s, f], mix_u + s)
    along(u_at, zu)
    forward(q_at, zq, yq, 3)
    forward(o_at, zo, yo, 3)
    across_own(u_at, yu)
    ag_forward(N1, ag1)
    ag_start(COT, agc)
    forward(u_at, zu, yu, 1, 1)
    along(d_at, zd)
    gathered(q_at, yq)
    for n, b in enumerate(order):
        if n in (1, 3):
            ag_wait(N1, ag1, b)
        QKV[lines(b), :] = dot(N1[b], WQ[...].reshape(width, 3 * part), 1, 0).astype(bf16)
    attn_fwd_kernel(lens, QKV, ATT, LSE)
    ag_forward(COT, agc)
    gathered(o_at, yo)

    def proj(b):
        PA[b] = dot(ATT[lines(b), :], WO[...].reshape(part, width), 1, 0).astype(bf16)

    proj_sends = len(sent)
    rs_send(PA, LA1, LA2, rs1, proj)
    proj_sends = sent[proj_sends:]
    forward(u_at, zu, yu, 2)
    forward(d_at, zd, yd, 1, 1)
    MID[...] = frames[...].astype(f32) + rs_total(PA, LA1, LA2, rs1)
    norm_rows(MID[...], N2F, INV2)
    NORM2[d] = (N2F[...] * VEC[2:3, :] + VEC[3:4, :]).astype(bf16)
    ag_start(NORM2, ag2)
    gathered(u_at, yu)

    def wide(i):
        return pl.ds(pl.multiple_of(i * 2 * part, part), 2 * part)

    def halves(step):
        lax.fori_loop(0, dpn // 2, lambda i, carry: (step(i), carry)[1], 0)

    def up(b):
        def half(i):
            u = dot(NORM2[b], WU[:, :, :, wide(i)].reshape(width, 2 * part), 1, 0)
            cdf = 0.5 * (1.0 + lax.erf(u * (0.5**0.5)))
            ACT[b, :, wide(i)] = (u * cdf).astype(bf16)
            SLOPE[b, :, wide(i)] = cdf + u * (jnp.exp(-0.5 * u * u) * (1.0 / (2.0 * jnp.pi) ** 0.5))

        halves(half)

    up(d)
    forward(d_at, zd, yd, 2, 2)
    ag_wait(NORM2, ag2, core)
    up(core)
    forward(d_at, zd, yd, 3)
    ag_forward(NORM2, ag2)
    up(far)
    ag_wait(NORM2, ag2, other)
    up(other)
    ag_wait(COT, agc, core)
    ag_wait(COT, agc, other)
    y_d, y_u, y_o, y_q = slots(nz), slots(dpn), slots(1), slots(dpn)
    z_d, z_u, z_o, z_q = slots(nz), slots(nz * dpn), slots(nz), slots(nz * dpn)
    big = wd_in.shape[0]

    def against(a, b, i):
        return dot(a[:, :, pl.ds(pl.multiple_of(i * part, part), part)].reshape(dpn * own, part), b, 0, 0).astype(bf16)

    def grad_down(k):
        GD[zpeer(k + 1)] = against(ACT, COT[...].reshape(dpn * own, width), zpeer(k + 1)).reshape(2, big, width)

    push_each(nz, lambda k: (GD.at[zpeer(k + 1), 1 - y], YD.at[zpeer(k + 1)], y_d + zpeer(k + 1), pair), grad_down)
    gathered(d_at, yd)
    per = fsn // dpn

    def grad_hidden(b):
        for i in range(dpn):
            g = dot(COT[b], WD[i * per : (i + 1) * per].reshape(part, width), 1, 1)
            GUP[b, :, tile(i)] = (g * SLOPE[b, :, tile(i)]).astype(bf16)
        for i in range(dpn):
            PB[b, :, tile(i)] = dot(GUP[b], WU[i].reshape(part, width), 1, 1).astype(bf16)

    norm2_sends = len(sent)
    rs_send(PB, LB1, LB2, rs2, grad_hidden)
    norm2_sends = sent[norm2_sends:]

    def add(a, b):
        return (a.astype(f32) + b.astype(f32)).astype(bf16)

    def sum_d(k):
        j = zpeer(k)
        arrive(YD.at[j], y_d + j)
        YD[j] = add(GD[j, y], YD[j])
        if k < nz:
            push(YD.at[j], ZD.at[z], z_d + z, (d, j * 2 + y))

    def sum_chunk(G, Y, S, Z, ys, zs, i):
        arrive(Y.at[i], ys + i)
        S[:, i] = add(G[i, :, y], Y[i])
        for k in range(1, nz):
            zz = zpeer(k)
            push(S.at[zz, i], Z.at[z, i], zs + z * dpn + i, (d, zz * 2 + y))

    def sum_u(i):
        sum_chunk(GU, YU, SU, ZU, y_u, z_u, i)

    def sum_q(i):
        sum_chunk(GQ, YQ, SQ, ZQ, y_q, z_q, i)

    sum_d(1)
    sent_out(proj_sends)

    def down(b):
        def half(i):
            PA[b, :, wide(i)] = dot(ACT[b], WD[:, :, wide(i)].reshape(width, 2 * part), 1, 0).astype(bf16)

        halves(half)

    rs_near(PA, LC1, rs3, down)
    sum_d(2)
    MIDG = N2F
    grad2 = rs_total(PB, LB1, LB2, rs2)
    mid_norm, gain2, bias2 = norm_back(N2F[...], INV2[...], VEC[2:3, :], grad2)
    MIDG[...] = cot[...].astype(f32) + mid_norm
    GPROJ[d] = MIDG[...].astype(bf16)
    ag_start(GPROJ, agp)
    sum_d(3)

    def grad_up(i):
        GU[i] = against(NORM2, GUP[...].reshape(dpn * own, width), i).reshape(nz, 2, rows, width)

    push_each(dpn, lambda i: (GU.at[i, :, 1 - y], YU.at[i], y_u + i, pair), grad_up)

    GATT, GQKV = GUP.at[:, :, :part], ACT.at[:, :, : 3 * part]
    DK, DV = SLOPE.at[:, :, :part], SLOPE.at[:, :, part : 2 * part]

    def grad_heads(b):
        GATT[b] = dot(GPROJ[b], WO[...].reshape(part, width), 1, 1).astype(bf16)

    grad_heads(d)
    ag_forward(GPROJ, agp)
    rs_far(PA, LC1, LC2, rs3)
    grad_heads(far)
    ag_wait(GPROJ, agp, core)
    grad_heads(core)
    ag_wait(GPROJ, agp, other)
    grad_heads(other)

    g = dot(ATT[...], GPROJ[...].reshape(dpn * own, width), 0, 0).astype(bf16)
    GO[...] = g.reshape(nz, 2, rows, width)
    push(GO.at[:, 1 - y], YO, y_o, pair)
    sum_d(nz)
    sum_u(0)

    attn_bwd_kernel(lens, QKV, GATT, LSE, GQKV, DK, DV, {2: lambda: sum_u(1), 1: lambda: sum_u(2), 0: lambda: sum_u(3)})

    def grad_q(i):
        GQ[i] = against(N1, GQKV[...].reshape(dpn * own, 3 * part), i).reshape(nz, 2, rows, 3 * part)

    push_each(dpn, lambda i: (GQ.at[i, :, 1 - y], YQ.at[i], y_q + i, pair), grad_q)

    sent_out(norm2_sends)

    def grad_first(b):
        def half(i):
            PB[b, :, wide(i)] = dot(GQKV[b], WQ[pl.ds(2 * i, 2)].reshape(2 * part, 3 * part), 1, 1).astype(bf16)

        halves(half)

    rs_send(PB, LD1, LD2, rs4, grad_first)

    arrive(YO, y_o)
    YO[...] = add(GO[:, y], YO[...])
    for k in range(1, nz):
        zz = zpeer(k)
        push(YO.at[zz], ZO.at[z], z_o + z, (d, zz * 2 + y))
    for i in range(dpn // 2):
        sum_q(i)
    grad1 = rs_total(PB, LD1, LD2, rs4)
    in_norm, gain1, bias1 = norm_back(N1F[...], INV1[...], VEC[0:1, :], grad1)
    o_in[...] = MIDG[...] + in_norm
    small = jnp.concatenate([v.reshape(1, width) for v in (gain1, bias1, gain2, bias2)] + [jnp.zeros((4, width), f32)], axis=0)
    for i in range(dpn):
        SM[i] = small[:, tile(i)]
    sm_d, sm_y, sm_z = slots(dpn), slots(1), slots(nz)
    for k in range(1, dpn):
        dd = lax.rem(d + k, dpn)
        push(SM.at[dd], SM1.at[d], sm_d + d, (dd, f))

    for i in range(dpn // 2, dpn):
        sum_q(i)
    SD, SO = YD, YO

    def settle(S, Z, zs, pieces=1):
        total = S[z].astype(f32)
        for k in range(1, nz):
            zz = zpeer(k)
            for i in range(pieces):
                arrive(Z.at[zz, i] if pieces > 1 else Z.at[zz], zs + zz * pieces + i)
            total = total + Z[zz].astype(f32)
        return total

    TU, TQ = GUP.at[:, :rows], GUP.at[:, rows : 2 * rows, : 3 * part]
    back_u, back_q = slots(dpn), slots(dpn)
    TU[...] = settle(SU, ZU, z_u, dpn).astype(bf16)
    for k in range(1, dpn):
        dd = lax.rem(d + k, dpn)
        push(TU.at[dd], RU.at[d], back_u + d, (dd, f))
    RU[d] = TU[d]

    o_d[...] = settle(SD, ZD, z_d)
    o_o[...] = settle(SO, ZO, z_o)

    total = SM[d]
    for k in range(1, dpn):
        s = lax.rem(d + k, dpn)
        arrive(SM1.at[s], sm_d + s)
        total = total + SM1[s]
    SM2[...] = total
    push(SM2, SM3, sm_y, pair)

    arrive(SM3, sm_y)
    SM4[...] = SM2[...] + SM3[...]
    for k in range(1, nz):
        push(SM4, SM5.at[z], sm_z + z, (d, zpeer(k) * 2 + y))

    TQ[...] = settle(SQ, ZQ, z_q, dpn).astype(bf16)
    for k in range(1, dpn):
        dd = lax.rem(d + k, dpn)
        push(TQ.at[dd], RQ.at[d], back_q + d, (dd, f))
    RQ[d] = TQ[d]

    o_res[...] = (MID[...] + rs_total(PA, LC1, LC2, rs3)).astype(bf16)
    for k in range(1, dpn):
        s = lax.rem(d + k, dpn)
        arrive(RU.at[s], back_u + s)
    for s in range(dpn):
        o_u[:, s * width : (s + 1) * width] = RU[s].astype(f32)
    for k in range(1, dpn):
        s = lax.rem(d + k, dpn)
        arrive(RQ.at[s], back_q + s)
    for s in range(dpn):
        for j in range(3):
            o_q[:, j * width + s * part : j * width + (s + 1) * part] = RQ[s, :, tile(j)].astype(f32)
    total = SM4[...]
    for k in range(1, nz):
        zz = zpeer(k)
        arrive(SM5.at[zz], sm_z + zz)
        total = total + SM5[zz]
    o_small[...] = total

    waited = set(id(copy) for _, copy in proj_sends + norm2_sends)
    sent_out([(when, copy) for when, copy in sent if id(copy) not in waited])


def in_one_kernel(frames, cotangent, phon_len, acou_len, row_item, w_qkv, w_out, w_up, w_down, ln1_gain, ln1_bias, ln2_gain, ln2_bias):
    dpn, fsn = lax.axis_size("dp"), lax.axis_size("fsdp")
    nz = fsn // 2
    own, width = frames.shape[1:]
    length = dpn * own
    part = width // dpn
    rows = w_up.shape[0]
    big = w_down.shape[0]
    place = lax.axis_index("fsdp") * rows % 128
    vec = jnp.stack([ln1_gain, ln1_bias, ln2_gain, ln2_bias]).astype(f32)
    vec = jnp.pad(vec, ((0, 4), (0, 128 - rows)))
    vec = jnp.roll(vec, place, axis=1)

    def buf(*shape, dtype=bf16):
        return pltpu.VMEM(shape, dtype)

    full = buf(dpn, own, width)
    land = [buf(2, own, width), buf(own, width)]
    scratch = [
        buf(dpn, fsn, 8, 128, dtype=f32), buf(8, width, dtype=f32),
        buf(dpn, fsn, rows, 3 * part), buf(fsn, rows, width), buf(dpn, fsn, rows, width), buf(fsn, big, width),
        buf(own, width, dtype=f32), buf(own, 1, dtype=f32), full, full,
        buf(length, 3 * part), buf(length, part), buf(8, length, dtype=f32), full, full,
        *land, *land, *land, *land,
        buf(own, width, dtype=f32), buf(own, width, dtype=f32), buf(own, 1, dtype=f32),
        full, full, buf(dpn, own, width, dtype=f32), full, full,
        buf(nz, 2, big, width), buf(dpn, nz, 2, rows, width), buf(nz, 2, rows, width), buf(dpn, nz, 2, rows, 3 * part),
        buf(nz, big, width), buf(dpn, nz, rows, width), buf(nz, rows, width), buf(dpn, nz, rows, 3 * part),
        buf(nz, dpn, rows, width), buf(nz, dpn, rows, 3 * part),
        buf(nz, big, width), buf(nz, dpn, rows, width), buf(nz, rows, width), buf(nz, dpn, rows, 3 * part),
        buf(dpn, rows, width), buf(dpn, rows, 3 * part),
        buf(dpn, 8, part, dtype=f32), buf(dpn, 8, part, dtype=f32), buf(8, part, dtype=f32), buf(8, part, dtype=f32),
        buf(8, part, dtype=f32), buf(nz, 8, part, dtype=f32),
        pltpu.SemaphoreType.DMA((SENDS,)), pltpu.SemaphoreType.DMA((ARRIVALS,)),
    ]
    outs = pl.pallas_call(
        layer_kernel,
        out_shape=(
            jax.ShapeDtypeStruct((own, width), bf16),
            jax.ShapeDtypeStruct((own, width), f32),
            jax.ShapeDtypeStruct((rows, 3 * width), f32),
            jax.ShapeDtypeStruct((rows, width), f32),
            jax.ShapeDtypeStruct((rows, dpn * width), f32),
            jax.ShapeDtypeStruct((big, width), f32),
            jax.ShapeDtypeStruct((8, part), f32),
        ),
        in_specs=[SMEM] * 3 + [VMEM] * 7,
        out_specs=(VMEM,) * 7,
        scratch_shapes=scratch,
        compiler_params=pltpu.CompilerParams(collective_id=0, has_side_effects=True, vmem_limit_bytes=67043328),
        name="layer",
    )(phon_len, acou_len, row_item, frames[0], cotangent[0], vec, w_qkv, w_out, w_up, w_down)
    small = lax.dynamic_slice(outs[6], (0, lax.axis_index("fsdp") * rows), (4, rows))
    return (outs[0][None], outs[1][None], *outs[2:6], small[0], small[1], small[2], small[3])


def on_device(*args):
    dpn, fsn, rows, width = lax.axis_size("dp"), lax.axis_size("fsdp"), args[7].shape[0], args[0].shape[2]
    fits = dpn == 4 and args[0].shape[1] == BLOCK and fsn % dpn == 0 and rows % 16 == 0 and 128 % rows == 0 and width == 2 * dpn * args[8].shape[0]
    return (in_one_kernel if fits else with_collectives)(*args)


def solution(mesh):
    split = P(("dp", "fsdp"), None)
    vec = P(("dp", "fsdp"))
    acts = P("fsdp", "dp", None)
    return jax.shard_map(
        on_device,
        mesh=mesh,
        in_specs=(acts, acts, P(), P(), P("fsdp"), split, split, split, split, vec, vec, vec, vec),
        out_specs=(acts, acts, split, split, split, split, vec, vec, vec, vec),
        check_vma=False,
    )
```

```python
import functools

import jax
import jax.numpy as jnp
from jax import lax
from jax.experimental import pallas as pl
from jax.experimental.pallas import tpu as pltpu
from jax.sharding import PartitionSpec as P

HEAD_DIM = 64
EPS = 1e-05
MASKED = -1e30
BLOCK = 256

f32 = jnp.float32
bf16 = jnp.bfloat16


def dot(a, b, ca, cb):
    return lax.dot_general(a, b, (((ca,), (cb,)), ((), ())), preferred_element_type=f32)


def row_limit(start, rows, phon, acou):
    pos = start + lax.broadcasted_iota(jnp.int32, (1, rows), 1)
    return jnp.where(pos < phon + acou, jnp.maximum(pos, phon - 1), phon - 1)


def head_mask(width, head):
    lane = lax.broadcasted_iota(jnp.int32, (1, width), 1)
    return (lane >= head * HEAD_DIM) & (lane < (head + 1) * HEAD_DIM)


def attn_fwd_kernel(lens, qkv, out, lse, between={}):
    width = out.shape[1]
    heads = width // HEAD_DIM
    length = out.shape[0]
    phon, acou = lens[0], lens[1]
    scale = HEAD_DIM ** (-0.5)
    for start in range(0, length, BLOCK):
        if start // BLOCK in between:
            between[start // BLOCK]()
        seen = start + BLOCK
        q = qkv[start : start + BLOCK, :width] * scale
        k = qkv[:seen, width : 2 * width]
        v = qkv[:seen, 2 * width :]
        limit = row_limit(start, BLOCK, phon, acou)
        key = lax.broadcasted_iota(jnp.int32, (seen, 1), 0)
        hidden = key > limit
        total = jnp.zeros((BLOCK, width), f32)
        rows = []
        for h in range(heads):
            mine = head_mask(width, h)
            qh = jnp.where(mine, q, 0)
            s = dot(k, qh, 1, 1)
            s = jnp.where(hidden, MASKED, s)
            top = jnp.max(s, axis=0, keepdims=True)
            e = jnp.exp(s - top)
            tot = jnp.sum(e, axis=0, keepdims=True)
            p = (e * (1.0 / tot)).astype(bf16)
            o = dot(p, v, 0, 0)
            total = total + jnp.where(mine, o, 0)
            rows.append(top + jnp.log(tot))
        out[start : start + BLOCK, :] = total.astype(bf16)
        lse[:, start : start + BLOCK] = jnp.concatenate(rows + [jnp.zeros((8 - heads, BLOCK), f32)], axis=0)


def attn_bwd_kernel(lens, qkv, grad, lse, dqkv, dk_acc, dv_acc, between={}):
    width = grad.shape[2]
    heads = width // HEAD_DIM
    length = grad.shape[0] * BLOCK
    phon, acou = lens[0], lens[1]
    scale = HEAD_DIM ** (-0.5)
    dk_acc[...] = jnp.zeros_like(dk_acc)
    dv_acc[...] = jnp.zeros_like(dv_acc)
    for start in reversed(range(0, length, BLOCK)):
        if start // BLOCK in between:
            between[start // BLOCK]()
        seen = start + BLOCK
        limit = row_limit(start, BLOCK, phon, acou)

        def two_heads(two, dq):
            q = qkv[start : start + BLOCK, :width] * scale
            g = grad[start // BLOCK]
            k = qkv[:seen, width : 2 * width]
            v = qkv[:seen, 2 * width :]
            hidden = lax.broadcasted_iota(jnp.int32, (seen, 1), 0) > limit
            for h in (2 * two, 2 * two + 1):
                mine = head_mask(width, h)
                qh = jnp.where(mine, q, 0)
                gh = jnp.where(mine, g, 0)
                s = dot(k, qh, 1, 1)
                s = jnp.where(hidden, MASKED, s)
                p = jnp.exp(s - lse[pl.ds(h, 1), start : start + BLOCK])
                gp = dot(v, gh, 1, 1)
                delta = jnp.sum(p * gp, axis=0, keepdims=True)
                ds = (p * (gp - delta)).astype(bf16)
                dvh = dot(p.astype(bf16), gh, 1, 0)
                dkh = dot(ds, qh, 1, 0)
                dv_acc[: seen // BLOCK] += dvh.reshape(seen // BLOCK, BLOCK, width)
                dk_acc[: seen // BLOCK] += dkh.reshape(seen // BLOCK, BLOCK, width)
                dq = dq + jnp.where(mine, dot(ds, k, 0, 0), 0)
            return dq

        dq = lax.fori_loop(0, heads // 2, two_heads, jnp.zeros((BLOCK, width), f32))
        dqkv[start // BLOCK, :, :width] = (dq * scale).astype(bf16)
    dqkv[:, :, width : 2 * width] = dk_acc[...].astype(bf16)
    dqkv[:, :, 2 * width :] = dv_acc[...].astype(bf16)


VMEM = pl.BlockSpec(memory_space=pltpu.VMEM)
SMEM = pl.BlockSpec(memory_space=pltpu.SMEM)


def attn_fwd(lens, qkv):
    length, width = qkv.shape[0], qkv.shape[1] // 3
    return pl.pallas_call(
        attn_fwd_kernel,
        out_shape=(jax.ShapeDtypeStruct((length, width), bf16), jax.ShapeDtypeStruct((8, length), f32)),
        in_specs=[SMEM, VMEM],
        out_specs=(VMEM, VMEM),
        compiler_params=pltpu.CompilerParams(vmem_limit_bytes=40 * 2**20),
        cost_estimate=pl.CostEstimate(flops=4 * length * length * width, bytes_accessed=8 * length * width, transcendentals=length * length * width // HEAD_DIM),
        name="attn_fwd",
    )(lens, qkv)


def attn_bwd(lens, qkv, grad, lse):
    length, width = grad.shape
    blocks = length // BLOCK
    out = pl.pallas_call(
        attn_bwd_kernel,
        out_shape=jax.ShapeDtypeStruct((blocks, BLOCK, 3 * width), bf16),
        in_specs=[SMEM, VMEM, VMEM, VMEM],
        out_specs=VMEM,
        scratch_shapes=[pltpu.VMEM((blocks, BLOCK, width), f32)] * 2,
        compiler_params=pltpu.CompilerParams(vmem_limit_bytes=40 * 2**20),
        cost_estimate=pl.CostEstimate(flops=10 * length * length * width, bytes_accessed=14 * length * width, transcendentals=length * length * width // HEAD_DIM),
        name="attn_bwd",
    )(lens, qkv, grad.reshape(blocks, BLOCK, width), lse)
    return out.reshape(length, 3 * width)


def norm_parts(v):
    mean = jnp.mean(v, axis=-1, keepdims=True)
    centered = v - mean
    var = jnp.mean(centered * centered, axis=-1, keepdims=True)
    inv = lax.rsqrt(var + EPS)
    return centered * inv, inv


def norm_back(n, inv, gain, grad):
    g = grad * gain
    dx = inv * (g - jnp.mean(g, axis=-1, keepdims=True) - n * jnp.mean(g * n, axis=-1, keepdims=True))
    return dx, jnp.sum(grad * n, axis=0), jnp.sum(grad, axis=0)


def with_collectives(frames, cotangent, phon_len, acou_len, row_item, w_qkv, w_out, w_up, w_down, ln1_gain, ln1_bias, ln2_gain, ln2_bias):
    tp, dpn, fsn = "dp", lax.axis_size("dp"), lax.axis_size("fsdp")
    width = frames.shape[2]
    part = width // dpn
    rows = w_up.shape[0]

    vecs = jnp.concatenate([ln1_gain, ln1_bias, ln2_gain, ln2_bias])[None]
    vecs = lax.all_gather(vecs, ("dp", "fsdp"), axis=0, tiled=True)
    vecs = vecs.reshape(dpn * fsn, 4, rows).transpose(1, 0, 2).reshape(4, width).astype(f32)

    qkv_cols = w_qkv.reshape(rows, 3, dpn, part).transpose(2, 0, 1, 3).reshape(dpn, rows, 3 * part)
    qkv_cols = lax.all_to_all(qkv_cols, tp, 0, 0, tiled=True)
    wq = lax.all_gather(qkv_cols, "fsdp", axis=1, tiled=True).reshape(width, 3 * part)
    wo = lax.all_gather(w_out, "fsdp", axis=0, tiled=True)
    ff = w_up.shape[1] // dpn
    up_cols = w_up.reshape(rows, dpn, ff).transpose(1, 0, 2)
    up_cols = lax.all_to_all(up_cols, tp, 0, 0, tiled=True)
    wu = lax.all_gather(up_cols, "fsdp", axis=1, tiled=True).reshape(width, ff)
    wd = lax.all_gather(w_down, "fsdp", axis=0, tiled=True)

    item = row_item[0]
    pick = jnp.arange(phon_len.shape[0], dtype=jnp.int32) == item
    lens = jnp.stack([jnp.sum(jnp.where(pick, phon_len, 0)), jnp.sum(jnp.where(pick, acou_len, 0))])

    x = frames[0].astype(f32)
    n1, inv1 = norm_parts(x)
    normed1 = lax.all_gather((n1 * vecs[0] + vecs[1]).astype(bf16), tp, axis=0, tiled=True)
    grad_down = lax.all_gather(cotangent[0], tp, axis=0, tiled=True)
    qkv = jnp.dot(normed1, wq, preferred_element_type=f32).astype(bf16)
    attn_out, lse = attn_fwd(lens, qkv)
    proj = jnp.dot(attn_out, wo, preferred_element_type=f32).astype(bf16)
    middle = x + lax.psum_scatter(proj, tp, scatter_dimension=0, tiled=True).astype(f32)
    n2, inv2 = norm_parts(middle)
    normed2 = lax.all_gather((n2 * vecs[2] + vecs[3]).astype(bf16), tp, axis=0, tiled=True)
    up_out = jnp.dot(normed2, wu, preferred_element_type=f32)
    cdf = 0.5 * (1.0 + lax.erf(up_out * (0.5**0.5)))
    act_out = (up_out * cdf).astype(bf16)
    down = jnp.dot(act_out, wd, preferred_element_type=f32).astype(bf16)
    result = (middle + lax.psum_scatter(down, tp, scatter_dimension=0, tiled=True).astype(f32)).astype(bf16)

    g_down = dot(act_out, grad_down, 0, 0).astype(bf16)
    slope = cdf + up_out * (jnp.exp(-0.5 * up_out * up_out) * (1.0 / (2.0 * jnp.pi) ** 0.5))
    grad_up = (dot(grad_down, wd, 1, 1) * slope).astype(bf16)
    g_up = dot(normed2, grad_up, 0, 0).astype(bf16)
    grad_norm2 = lax.psum_scatter(dot(grad_up, wu, 1, 1).astype(bf16), tp, scatter_dimension=0, tiled=True).astype(f32)
    mid_norm, g_gain2, g_bias2 = norm_back(n2, inv2, vecs[2], grad_norm2)
    grad_middle = cotangent[0].astype(f32) + mid_norm
    grad_proj = lax.all_gather(grad_middle.astype(bf16), tp, axis=0, tiled=True)
    g_out = dot(attn_out, grad_proj, 0, 0).astype(bf16)
    grad_attn = dot(grad_proj, wo, 1, 1).astype(bf16)
    grad_qkv = attn_bwd(lens, qkv, grad_attn, lse)
    g_qkv = dot(normed1, grad_qkv, 0, 0).astype(bf16)
    grad_norm1 = lax.psum_scatter(dot(grad_qkv, wq, 1, 1).astype(bf16), tp, scatter_dimension=0, tiled=True).astype(f32)
    in_norm, g_gain1, g_bias1 = norm_back(n1, inv1, vecs[0], grad_norm1)
    grad_inputs = grad_middle + in_norm

    def owned_rows(g):
        return lax.psum_scatter(g, "fsdp", scatter_dimension=0, tiled=True)

    def owned_cols(g, groups):
        g = lax.psum_scatter(g.reshape(dpn, width // dpn, -1), "fsdp", scatter_dimension=1, tiled=True)
        g = lax.all_to_all(g, tp, 0, 0, tiled=True)
        g = g.reshape(dpn, rows, groups, -1).transpose(1, 2, 0, 3)
        return g.reshape(rows, -1).astype(f32)

    o_down = owned_rows(g_down).astype(f32)
    o_up = owned_cols(g_up, 1)
    o_out = owned_rows(g_out).astype(f32)
    o_qkv = owned_cols(g_qkv, 3)
    small = jnp.stack([g_gain1, g_bias1, g_gain2, g_bias2]).reshape(4, dpn * fsn, rows).transpose(1, 0, 2)
    small = lax.psum_scatter(small.reshape(dpn * fsn, 4 * rows), ("dp", "fsdp"), scatter_dimension=0, tiled=True).reshape(4, rows)
    return (result[None], grad_inputs[None], o_qkv, o_out, o_up, o_down, small[0], small[1], small[2], small[3])


CHUNKS = 2
SENDS = 320
ARRIVALS = 320
MESH = pl.DeviceIdType.MESH


def layer_kernel(
    phon_len, acou_len, row_item, frames, cot, vec_in, wq_in, wo_in, wu_in, wd_in,
    o_res, o_in, o_q, o_o, o_u, o_d, o_small,
    VG, VEC, WQ, WO, WU, WD, N1F, INV1, N1, COT, QKV, ATT, LSE, PA, PB,
    LA1, LA2, LB1, LB2, LC1, LC2, LD1, LD2,
    MID, N2F, INV2, NORM2, ACT, SLOPE, GUP, GPROJ,
    GD, GU, GO, GQ, YD, YU, YO, YQ, SU, SQ, ZD, ZU, ZO, ZQ, RU, RQ,
    SM, SM1, SM2, SM3, SM4, SM5,
    ssem, rsem,
):
    dpn, fsn = lax.axis_size("dp"), lax.axis_size("fsdp")
    lens = (phon_len[row_item[0]], acou_len[row_item[0]])
    nz = fsn // 2
    width = frames.shape[1]
    own = frames.shape[0]
    part = width // dpn
    rows = wu_in.shape[0]
    d, f = lax.axis_index("dp"), lax.axis_index("fsdp")
    c, x = lax.rem(d, 2), lax.div(d, 2)
    y, z = lax.rem(f, 2), lax.div(f, 2)
    core = d + 1 - 2 * c
    far = lax.rem(d + 2, dpn)
    other = lax.rem(core + 2, dpn)
    order = (d, core, far, other)
    pair = (d, f + 1 - 2 * y)
    count = {"send": 0, "arrive": 0}
    sent = []

    def slots(n):
        base = count["arrive"]
        count["arrive"] += n
        assert count["arrive"] <= ARRIVALS
        return base

    def push(src, dst, slot, device, when=None):
        i = count["send"]
        count["send"] += 1
        assert i < SENDS
        copy = pltpu.make_async_remote_copy(src, dst, ssem.at[i], rsem.at[slot], device_id=device, device_id_type=MESH)
        if when is None:
            copy.start()
        else:
            pl.when(when)(lambda: copy.start())
        sent.append((when, copy))

    def push_each(n, piece, compute):
        first = count["send"]
        count["send"] += n

        def copy_of(i):
            src, dst, slot, device = piece(i)
            return pltpu.make_async_remote_copy(src, dst, ssem.at[first + i], rsem.at[slot], device_id=device, device_id_type=MESH)

        def step(i, carry):
            compute(i)
            copy_of(i).start()
            return carry

        lax.fori_loop(0, n, step, 0)
        sent.extend((None, copy_of(i)) for i in range(n))

    def sent_out(copies):
        for when, copy in copies:
            if when is None:
                copy.wait_send()
            else:
                pl.when(when)(lambda copy=copy: copy.wait_send())

    def arrive(ref, slot):
        pltpu.make_async_remote_copy(ref, ref, ssem.at[0], rsem.at[slot], device_id=pair, device_id_type=MESH).wait_recv()

    def zpeer(k):
        return lax.rem(z + k, nz)

    barrier = pltpu.get_barrier_semaphore()
    peers = [(lax.rem(d + k, dpn), f) for k in range(1, dpn)] + [(d, lax.rem(f + k, fsn)) for k in range(1, fsn)]
    for device in peers:
        pl.semaphore_signal(barrier, inc=1, device_id=device, device_id_type=MESH)
    pl.semaphore_wait(barrier, len(peers))

    def tile(i):
        return slice(i * part, (i + 1) * part)

    vec_f, vec_d = slots(fsn), slots(dpn)
    for k in range(1, fsn):
        push(vec_in, VG.at[d, f], vec_f + f, (d, lax.rem(f + k, fsn)))
    mix_q, mix_u = slots(dpn * 3), slots(dpn)

    def q_cols(dd, j):
        return pl.ds(pl.multiple_of(j * width + dd * part, part), part)

    def u_cols(dd):
        return pl.ds(pl.multiple_of(dd * width, width), width)

    for k in range(1, dpn):
        dd = lax.rem(d + k, dpn)
        for j in range(3):
            push(wq_in.at[:, q_cols(dd, j)], WQ.at[d, f, :, tile(j)], mix_q + d * 3 + j, (dd, f))
    for k in range(1, dpn):
        dd = lax.rem(d + k, dpn)
        push(wu_in.at[:, u_cols(dd)], WU.at[d, f], mix_u + d, (dd, f))
    zq, zo, zu, zd = slots(nz), slots(nz), slots(nz), slots(nz)
    yq, yo, yu, yd = slots(nz), slots(nz), slots(nz), slots(nz)
    def clip(v):
        return jnp.clip(v, 0, nz - 1)

    def along(ref_at, zs):
        for side in (1, -1):
            to = z + side
            push(ref_at(f), ref_at(f), zs + z, (d, clip(to) * 2 + y), when=(to >= 0) & (to < nz))

    def across_own(ref_at, ys):
        push(ref_at(f), ref_at(f), ys + z, pair)

    def hop(ref_at, zs, ys, h):
        for side in (1, -1):
            src, to = z + side * h, z - side
            here = (src >= 0) & (src < nz)
            ref, src = ref_at(clip(src) * 2 + y), clip(src)
            pl.when(here)(lambda: arrive(ref, zs + src))
            push(ref, ref, zs + src, (d, clip(to) * 2 + y), when=here & (to >= 0) & (to < nz))
            push(ref, ref, ys + src, pair, when=here)

    def forward(ref_at, zs, ys, first=1, last=None):
        for h in range(first, nz if last is None else last + 1):
            hop(ref_at, zs, ys, h)

    def gathered(ref_at, ys):
        for zz in range(nz):
            arrive(ref_at(2 * zz + 1 - y), ys + zz)

    def q_at(s):
        return WQ.at[:, s]

    def o_at(s):
        return WO.at[s]

    def u_at(s):
        return WU.at[:, s]

    def d_at(s):
        return WD.at[s]

    WO[f] = wo_in[...]
    WD[f] = wd_in[...]
    along(o_at, zo)
    across_own(o_at, yo)
    across_own(d_at, yd)
    VG[d, f] = vec_in[...]
    for j in range(3):
        WQ[d, f, :, tile(j)] = wq_in[:, q_cols(d, j)]
    WU[d, f] = wu_in[:, u_cols(d)]

    def norm_rows(v, nf, inv):
        n, i = norm_parts(v)
        nf[...] = n
        inv[...] = i

    norm_rows(frames[...].astype(f32), N1F, INV1)
    for k in range(1, fsn):
        s = lax.rem(f + k, fsn)
        arrive(VG.at[d, s], vec_f + s)
    for k in range(1, dpn):
        push(VG.at[d], VG.at[d], vec_d + d, (lax.rem(d + k, dpn), f))

    for k in range(1, dpn):
        s = lax.rem(d + k, dpn)
        for j in range(3):
            arrive(WQ.at[s, f, :, tile(j)], mix_q + s * 3 + j)
    along(q_at, zq)
    across_own(q_at, yq)
    for k in range(1, dpn):
        s = lax.rem(d + k, dpn)
        arrive(VG.at[s], vec_d + s)
    group = 128 // rows
    for m in range(width // 128):
        total = VG[(m * group) // fsn, (m * group) % fsn]
        for j in range(1, group):
            total = total + VG[(m * group + j) // fsn, (m * group + j) % fsn]
        VEC[:, m * 128 : (m + 1) * 128] = total

    step = own // CHUNKS

    def ag_start(ref, base):
        for device in (far, core):
            for h in range(CHUNKS):
                piece = ref.at[d, h * step : (h + 1) * step]
                push(piece, piece, base + d * CHUNKS + h, (device, f))

    def ag_forward(ref, base):
        for h in range(CHUNKS):
            piece = ref.at[far, h * step : (h + 1) * step]
            arrive(piece, base + far * CHUNKS + h)
            push(piece, piece, base + far * CHUNKS + h, (core, f))

    def ag_wait(ref, base, b):
        for h in range(CHUNKS):
            arrive(ref.at[b, h * step : (h + 1) * step], base + b * CHUNKS + h)

    def rs_near(P, L1, base, compute, between=lambda: None):
        for j, hi in enumerate((1 - x, x)):
            b_send, b_keep = hi * 2 + 1 - c, hi * 2 + c
            compute(b_send)
            push(P.at[b_send], L1.at[j], base + j, (core, f))
            compute(b_keep)
            if j == 0:
                between()

    def rs_far(P, L1, L2, base):
        b_far = (1 - x) * 2 + c
        arrive(L1.at[0], base)
        P[b_far] = (P[b_far].astype(f32) + L1[0].astype(f32)).astype(bf16)
        push(P.at[b_far], L2, base + 2, (far, f))

    def rs_send(P, L1, L2, base, compute):
        rs_near(P, L1, base, compute, lambda: rs_far(P, L1, L2, base))

    def rs_total(P, L1, L2, base):
        arrive(L1.at[1], base + 1)
        arrive(L2, base + 2)
        return P[d].astype(f32) + L1[1].astype(f32) + L2[...].astype(f32)

    def lines(b):
        return pl.ds(pl.multiple_of(b * own, own), own)

    ag1, agc, ag2, agp = slots(dpn * CHUNKS), slots(dpn * CHUNKS), slots(dpn * CHUNKS), slots(dpn * CHUNKS)
    rs1, rs2, rs3, rs4 = slots(3), slots(3), slots(3), slots(3)

    N1[d] = (N1F[...] * VEC[0:1, :] + VEC[1:2, :]).astype(bf16)
    COT[d] = cot[...]
    ag_start(N1, ag1)
    forward(q_at, zq, yq, 1, 1)
    forward(o_at, zo, yo, 1, 1)
    forward(q_at, zq, yq, 2, 2)
    forward(o_at, zo, yo, 2, 2)
    for k in range(1, dpn):
        s = lax.rem(d + k, dpn)
        arrive(WU.at[s, f], mix_u + s)
    along(u_at, zu)
    forward(q_at, zq, yq, 3)
    forward(o_at, zo, yo, 3)
    across_own(u_at, yu)
    ag_forward(N1, ag1)
    ag_start(COT, agc)
    forward(u_at, zu, yu, 1, 1)
    along(d_at, zd)
    gathered(q_at, yq)
    for n, b in enumerate(order):
        if n in (1, 3):
            ag_wait(N1, ag1, b)
        QKV[lines(b), :] = dot(N1[b], WQ[...].reshape(width, 3 * part), 1, 0).astype(bf16)
    attn_fwd_kernel(lens, QKV, ATT, LSE)
    ag_forward(COT, agc)
    gathered(o_at, yo)

    def proj(b):
        PA[b] = dot(ATT[lines(b), :], WO[...].reshape(part, width), 1, 0).astype(bf16)

    proj_sends = len(sent)
    rs_send(PA, LA1, LA2, rs1, proj)
    proj_sends = sent[proj_sends:]
    forward(u_at, zu, yu, 2)
    forward(d_at, zd, yd, 1, 1)
    MID[...] = frames[...].astype(f32) + rs_total(PA, LA1, LA2, rs1)
    norm_rows(MID[...], N2F, INV2)
    NORM2[d] = (N2F[...] * VEC[2:3, :] + VEC[3:4, :]).astype(bf16)
    ag_start(NORM2, ag2)
    gathered(u_at, yu)

    def wide(i):
        return pl.ds(pl.multiple_of(i * 2 * part, part), 2 * part)

    def halves(step):
        lax.fori_loop(0, dpn // 2, lambda i, carry: (step(i), carry)[1], 0)

    def up(b):
        def half(i):
            u = dot(NORM2[b], WU[:, :, :, wide(i)].reshape(width, 2 * part), 1, 0)
            cdf = 0.5 * (1.0 + lax.erf(u * (0.5**0.5)))
            ACT[b, :, wide(i)] = (u * cdf).astype(bf16)
            SLOPE[b, :, wide(i)] = cdf + u * (jnp.exp(-0.5 * u * u) * (1.0 / (2.0 * jnp.pi) ** 0.5))

        halves(half)

    up(d)
    forward(d_at, zd, yd, 2, 2)
    ag_wait(NORM2, ag2, core)
    up(core)
    forward(d_at, zd, yd, 3)
    ag_forward(NORM2, ag2)
    up(far)
    ag_wait(NORM2, ag2, other)
    up(other)
    ag_wait(COT, agc, core)
    ag_wait(COT, agc, other)
    y_d, y_u, y_o, y_q = slots(nz), slots(dpn), slots(1), slots(dpn)
    z_d, z_u, z_o, z_q = slots(nz), slots(nz * dpn), slots(nz), slots(nz * dpn)
    big = wd_in.shape[0]

    def against(a, b, i):
        return dot(a[:, :, pl.ds(pl.multiple_of(i * part, part), part)].reshape(dpn * own, part), b, 0, 0).astype(bf16)

    def grad_down(k):
        GD[zpeer(k + 1)] = against(ACT, COT[...].reshape(dpn * own, width), zpeer(k + 1)).reshape(2, big, width)

    push_each(nz, lambda k: (GD.at[zpeer(k + 1), 1 - y], YD.at[zpeer(k + 1)], y_d + zpeer(k + 1), pair), grad_down)
    gathered(d_at, yd)
    per = fsn // dpn

    def grad_hidden(b):
        for i in range(dpn):
            g = dot(COT[b], WD[i * per : (i + 1) * per].reshape(part, width), 1, 1)
            GUP[b, :, tile(i)] = (g * SLOPE[b, :, tile(i)]).astype(bf16)
        for i in range(dpn):
            PB[b, :, tile(i)] = dot(GUP[b], WU[i].reshape(part, width), 1, 1).astype(bf16)

    norm2_sends = len(sent)
    rs_send(PB, LB1, LB2, rs2, grad_hidden)
    norm2_sends = sent[norm2_sends:]

    def add(a, b):
        return (a.astype(f32) + b.astype(f32)).astype(bf16)

    def sum_d(k):
        j = zpeer(k)
        arrive(YD.at[j], y_d + j)
        YD[j] = add(GD[j, y], YD[j])
        if k < nz:
            push(YD.at[j], ZD.at[z], z_d + z, (d, j * 2 + y))

    def sum_chunk(G, Y, S, Z, ys, zs, i):
        arrive(Y.at[i], ys + i)
        S[:, i] = add(G[i, :, y], Y[i])
        for k in range(1, nz):
            zz = zpeer(k)
            push(S.at[zz, i], Z.at[z, i], zs + z * dpn + i, (d, zz * 2 + y))

    def sum_u(i):
        sum_chunk(GU, YU, SU, ZU, y_u, z_u, i)

    def sum_q(i):
        sum_chunk(GQ, YQ, SQ, ZQ, y_q, z_q, i)

    sum_d(1)
    sent_out(proj_sends)

    def down(b):
        def half(i):
            PA[b, :, wide(i)] = dot(ACT[b], WD[:, :, wide(i)].reshape(width, 2 * part), 1, 0).astype(bf16)

        halves(half)

    rs_near(PA, LC1, rs3, down)
    sum_d(2)
    MIDG = N2F
    grad2 = rs_total(PB, LB1, LB2, rs2)
    mid_norm, gain2, bias2 = norm_back(N2F[...], INV2[...], VEC[2:3, :], grad2)
    MIDG[...] = cot[...].astype(f32) + mid_norm
    GPROJ[d] = MIDG[...].astype(bf16)
    ag_start(GPROJ, agp)
    sum_d(3)

    def grad_up(i):
        GU[i] = against(NORM2, GUP[...].reshape(dpn * own, width), i).reshape(nz, 2, rows, width)

    push_each(dpn, lambda i: (GU.at[i, :, 1 - y], YU.at[i], y_u + i, pair), grad_up)

    GATT, GQKV = GUP.at[:, :, :part], ACT.at[:, :, : 3 * part]
    DK, DV = SLOPE.at[:, :, :part], SLOPE.at[:, :, part : 2 * part]

    def grad_heads(b):
        GATT[b] = dot(GPROJ[b], WO[...].reshape(part, width), 1, 1).astype(bf16)

    grad_heads(d)
    ag_forward(GPROJ, agp)
    rs_far(PA, LC1, LC2, rs3)
    grad_heads(far)
    ag_wait(GPROJ, agp, core)
    grad_heads(core)
    ag_wait(GPROJ, agp, other)
    grad_heads(other)

    g = dot(ATT[...], GPROJ[...].reshape(dpn * own, width), 0, 0).astype(bf16)
    GO[...] = g.reshape(nz, 2, rows, width)
    push(GO.at[:, 1 - y], YO, y_o, pair)
    sum_d(nz)
    sum_u(0)

    attn_bwd_kernel(lens, QKV, GATT, LSE, GQKV, DK, DV, {2: lambda: sum_u(1), 1: lambda: sum_u(2), 0: lambda: sum_u(3)})

    def grad_q(i):
        GQ[i] = against(N1, GQKV[...].reshape(dpn * own, 3 * part), i).reshape(nz, 2, rows, 3 * part)

    push_each(dpn, lambda i: (GQ.at[i, :, 1 - y], YQ.at[i], y_q + i, pair), grad_q)

    sent_out(norm2_sends)

    def grad_first(b):
        def half(i):
            PB[b, :, wide(i)] = dot(GQKV[b], WQ[pl.ds(2 * i, 2)].reshape(2 * part, 3 * part), 1, 1).astype(bf16)

        halves(half)

    rs_send(PB, LD1, LD2, rs4, grad_first)

    arrive(YO, y_o)
    YO[...] = add(GO[:, y], YO[...])
    for k in range(1, nz):
        zz = zpeer(k)
        push(YO.at[zz], ZO.at[z], z_o + z, (d, zz * 2 + y))
    for i in range(dpn // 2):
        sum_q(i)
    grad1 = rs_total(PB, LD1, LD2, rs4)
    in_norm, gain1, bias1 = norm_back(N1F[...], INV1[...], VEC[0:1, :], grad1)
    o_in[...] = MIDG[...] + in_norm
    small = jnp.concatenate([v.reshape(1, width) for v in (gain1, bias1, gain2, bias2)] + [jnp.zeros((4, width), f32)], axis=0)
    for i in range(dpn):
        SM[i] = small[:, tile(i)]
    sm_d, sm_y, sm_z = slots(dpn), slots(1), slots(nz)
    for k in range(1, dpn):
        dd = lax.rem(d + k, dpn)
        push(SM.at[dd], SM1.at[d], sm_d + d, (dd, f))

    for i in range(dpn // 2, dpn):
        sum_q(i)
    SD, SO = YD, YO

    def settle(S, Z, zs, pieces=1):
        total = S[z].astype(f32)
        for k in range(1, nz):
            zz = zpeer(k)
            for i in range(pieces):
                arrive(Z.at[zz, i] if pieces > 1 else Z.at[zz], zs + zz * pieces + i)
            total = total + Z[zz].astype(f32)
        return total

    TU, TQ = GUP.at[:, :rows], GUP.at[:, rows : 2 * rows, : 3 * part]
    back_u, back_q = slots(dpn), slots(dpn)
    TU[...] = settle(SU, ZU, z_u, dpn).astype(bf16)
    for k in range(1, dpn):
        dd = lax.rem(d + k, dpn)
        push(TU.at[dd], RU.at[d], back_u + d, (dd, f))
    RU[d] = TU[d]

    o_d[...] = settle(SD, ZD, z_d)
    o_o[...] = settle(SO, ZO, z_o)

    total = SM[d]
    for k in range(1, dpn):
        s = lax.rem(d + k, dpn)
        arrive(SM1.at[s], sm_d + s)
        total = total + SM1[s]
    SM2[...] = total
    push(SM2, SM3, sm_y, pair)

    arrive(SM3, sm_y)
    SM4[...] = SM2[...] + SM3[...]
    for k in range(1, nz):
        push(SM4, SM5.at[z], sm_z + z, (d, zpeer(k) * 2 + y))

    TQ[...] = settle(SQ, ZQ, z_q, dpn).astype(bf16)
    for k in range(1, dpn):
        dd = lax.rem(d + k, dpn)
        push(TQ.at[dd], RQ.at[d], back_q + d, (dd, f))
    RQ[d] = TQ[d]

    o_res[...] = (MID[...] + rs_total(PA, LC1, LC2, rs3)).astype(bf16)
    for k in range(1, dpn):
        s = lax.rem(d + k, dpn)
        arrive(RU.at[s], back_u + s)
    for s in range(dpn):
        o_u[:, s * width : (s + 1) * width] = RU[s].astype(f32)
    for k in range(1, dpn):
        s = lax.rem(d + k, dpn)
        arrive(RQ.at[s], back_q + s)
    for s in range(dpn):
        for j in range(3):
            o_q[:, j * width + s * part : j * width + (s + 1) * part] = RQ[s, :, tile(j)].astype(f32)
    total = SM4[...]
    for k in range(1, nz):
        zz = zpeer(k)
        arrive(SM5.at[zz], sm_z + zz)
        total = total + SM5[zz]
    o_small[...] = total

    waited = set(id(copy) for _, copy in proj_sends + norm2_sends)
    sent_out([(when, copy) for when, copy in sent if id(copy) not in waited])


def copy_kernel(*refs):
    n = (len(refs) - 1) // 3
    ins, outs, held, sem = refs[:n], refs[n : 2 * n], refs[2 * n : 3 * n], refs[3 * n]
    first = [pltpu.make_async_copy(a, h, sem.at[0, i]) for i, (a, h) in enumerate(zip(ins, held))]
    second = [pltpu.make_async_copy(h, o, sem.at[1, i]) for i, (h, o) in enumerate(zip(held, outs))]
    for copy in first:
        copy.start()
    for one, two in zip(first, second):
        one.wait()
        two.start()
    for copy in second:
        copy.wait()


def copied(arrays):
    anywhere = pl.BlockSpec(memory_space=pl.ANY)
    return pl.pallas_call(
        copy_kernel,
        out_shape=tuple(jax.ShapeDtypeStruct(a.shape, a.dtype) for a in arrays),
        in_specs=[anywhere] * len(arrays),
        out_specs=(anywhere,) * len(arrays),
        scratch_shapes=[pltpu.VMEM(a.shape, a.dtype) for a in arrays] + [pltpu.SemaphoreType.DMA((2, len(arrays)))],
        name="results",
    )(*arrays)


def in_one_kernel(frames, cotangent, phon_len, acou_len, row_item, w_qkv, w_out, w_up, w_down, ln1_gain, ln1_bias, ln2_gain, ln2_bias):
    dpn, fsn = lax.axis_size("dp"), lax.axis_size("fsdp")
    nz = fsn // 2
    own, width = frames.shape[1:]
    length = dpn * own
    part = width // dpn
    rows = w_up.shape[0]
    big = w_down.shape[0]
    place = lax.axis_index("fsdp") * rows % 128
    vec = jnp.stack([ln1_gain, ln1_bias, ln2_gain, ln2_bias]).astype(f32)
    vec = jnp.pad(vec, ((0, 4), (0, 128 - rows)))
    vec = jnp.roll(vec, place, axis=1)

    def buf(*shape, dtype=bf16):
        return pltpu.VMEM(shape, dtype)

    full = buf(dpn, own, width)
    land = [buf(2, own, width), buf(own, width)]
    scratch = [
        buf(dpn, fsn, 8, 128, dtype=f32), buf(8, width, dtype=f32),
        buf(dpn, fsn, rows, 3 * part), buf(fsn, rows, width), buf(dpn, fsn, rows, width), buf(fsn, big, width),
        buf(own, width, dtype=f32), buf(own, 1, dtype=f32), full, full,
        buf(length, 3 * part), buf(length, part), buf(8, length, dtype=f32), full, full,
        *land, *land, *land, *land,
        buf(own, width, dtype=f32), buf(own, width, dtype=f32), buf(own, 1, dtype=f32),
        full, full, buf(dpn, own, width, dtype=f32), full, full,
        buf(nz, 2, big, width), buf(dpn, nz, 2, rows, width), buf(nz, 2, rows, width), buf(dpn, nz, 2, rows, 3 * part),
        buf(nz, big, width), buf(dpn, nz, rows, width), buf(nz, rows, width), buf(dpn, nz, rows, 3 * part),
        buf(nz, dpn, rows, width), buf(nz, dpn, rows, 3 * part),
        buf(nz, big, width), buf(nz, dpn, rows, width), buf(nz, rows, width), buf(nz, dpn, rows, 3 * part),
        buf(dpn, rows, width), buf(dpn, rows, 3 * part),
        buf(dpn, 8, part, dtype=f32), buf(dpn, 8, part, dtype=f32), buf(8, part, dtype=f32), buf(8, part, dtype=f32),
        buf(8, part, dtype=f32), buf(nz, 8, part, dtype=f32),
        pltpu.SemaphoreType.DMA((SENDS,)), pltpu.SemaphoreType.DMA((ARRIVALS,)),
    ]
    outs = pl.pallas_call(
        layer_kernel,
        out_shape=(
            jax.ShapeDtypeStruct((own, width), bf16),
            jax.ShapeDtypeStruct((own, width), f32),
            jax.ShapeDtypeStruct((rows, 3 * width), f32),
            jax.ShapeDtypeStruct((rows, width), f32),
            jax.ShapeDtypeStruct((rows, dpn * width), f32),
            jax.ShapeDtypeStruct((big, width), f32),
            jax.ShapeDtypeStruct((8, part), f32),
        ),
        in_specs=[SMEM] * 3 + [VMEM] * 7,
        out_specs=(VMEM,) * 7,
        scratch_shapes=scratch,
        compiler_params=pltpu.CompilerParams(collective_id=0, has_side_effects=True, vmem_limit_bytes=67043328),
        name="layer",
    )(phon_len, acou_len, row_item, frames[0], cotangent[0], vec, w_qkv, w_out, w_up, w_down)
    small = lax.dynamic_slice(outs[6], (0, lax.axis_index("fsdp") * rows), (4, rows))
    outs = copied(outs[:6])
    return (outs[0][None], outs[1][None], *outs[2:6], small[0], small[1], small[2], small[3])


def on_device(*args):
    dpn, fsn, rows, width = lax.axis_size("dp"), lax.axis_size("fsdp"), args[7].shape[0], args[0].shape[2]
    fits = dpn == 4 and args[0].shape[1] == BLOCK and fsn % dpn == 0 and rows % 16 == 0 and 128 % rows == 0 and width == 2 * dpn * args[8].shape[0]
    return (in_one_kernel if fits else with_collectives)(*args)


def solution(mesh):
    split = P(("dp", "fsdp"), None)
    vec = P(("dp", "fsdp"))
    acts = P("fsdp", "dp", None)
    return jax.shard_map(
        on_device,
        mesh=mesh,
        in_specs=(acts, acts, P(), P(), P("fsdp"), split, split, split, split, vec, vec, vec, vec),
        out_specs=(acts, acts, split, split, split, split, vec, vec, vec, vec),
        check_vma=False,
    )
```
